32 devices in a mesh: date: 16 (over z, y, x), pix: 2 (over core).
Axes of the slice: x: 2, y: 2, z: 4, core: 2. Of those that a mesh axis runs over, the one named last changes fastest.
Arguments:
- reflect: bfloat16 [64, 6, 16384], P('date', None, 'pix'), may hold values from -8 to 8
- cloud_free: int32 [64, 16384], P('date', 'pix'), may hold values from 0 to 1, as said below
- days: int32 [64], P('date'), may hold values from 1 to 2079, as said below
Outputs:
- median: float32 [6, 16384], P(None, 'pix')
- slope: float32 [6, 16384], P(None, 'pix')
The draws below stay inside these ranges and needn't reach their ends.
Inputs may be any that keep to these rules, and one draw needn't show every extreme that they name: `cloud_free`: every pixel is clear on at least one of the first 32 dates and on at least one of the others; clear shares differ between tiles. `days`: strictly increasing.
All inputs are finite; a program needn't handle non-finite values.
Results may differ from the reference program's by a relative error of at most 0.0003.
Values may be sent and summed in bfloat16 or wider, within the bound.
No kernel may reach another device: no remote copies, remote signals or barrier semaphores. Data moves between devices by JAX's collectives and lax.ppermute only.
A program may use at most 64 MiB of HBM per device.

```python
import jax
import jax.numpy as jnp
from jax import lax

DATES = 64
BANDS = 6
PIX_DEV = 8192
PIXELS = 16384


def draw_reflect(key, part):
    keys = jax.random.split(key, 4)
    tiles = PIXELS // PIX_DEV
    region = jax.random.normal(keys[0], (1, BANDS, tiles), jnp.float32)
    haze = 0.6 * jax.random.normal(keys[1], (DATES, BANDS, 1), jnp.float32)
    tile_date = 0.5 * jax.random.normal(keys[2], (DATES, BANDS, tiles), jnp.float32)
    base = jnp.repeat(region + tile_date, PIX_DEV, axis=2) + haze
    noise = 0.8 * jax.random.normal(keys[3], (DATES, BANDS, PIXELS), jnp.float32)
    return jnp.clip(base + noise, -8.0, 8.0).astype(jnp.bfloat16)


def draw_cloud_free(key, part):
    keys = jax.random.split(key, 4)
    tiles = PIXELS // PIX_DEV
    cloudy = jnp.repeat(jax.random.randint(keys[0], (tiles,), 10, 85), PIX_DEV)
    rolls = jax.random.randint(keys[1], (DATES, PIXELS), 0, 100)
    clear = rolls >= cloudy[None, :]
    first = jax.random.randint(keys[2], (PIXELS,), 0, DATES // 2)
    second = jax.random.randint(keys[3], (PIXELS,), DATES // 2, DATES)
    rows = jnp.arange(DATES, dtype=jnp.int32)[:, None]
    clear = clear | (rows == first[None, :]) | (rows == second[None, :])
    return clear.astype(jnp.int32)


def draw_days(key, part):
    keys = jax.random.split(key, 2)
    start = jax.random.randint(keys[0], (), 0, 31)
    gaps = jax.random.randint(keys[1], (DATES,), 1, 33)
    raw = (start + jnp.cumsum(gaps)).astype(jnp.int32)
    index = jnp.arange(DATES, dtype=jnp.int32)
    raw = jnp.where(index == 0, jnp.int32(1), raw)
    raw = jnp.where(index == DATES - 1, jnp.int32(31 + 32 * DATES), raw)
    return raw.astype(jnp.int32)


def setup_inputs(seed: int = 0) -> dict:
    arg_keys = jax.random.split(jax.random.key(seed), 4)
    reflect = draw_reflect(jax.random.fold_in(arg_keys[3], 71), 0)
    cloud_free = draw_cloud_free(jax.random.fold_in(arg_keys[3], 71), 0)
    days = draw_days(jax.random.fold_in(arg_keys[3], 71), 0)
    return {"reflect": reflect, "cloud_free": cloud_free, "days": days}


ridge = 1.0


def rank_block(pair):
    xb, mb = pair
    zeros = jnp.zeros(xb.shape, jnp.float32)

    def step(i, carry):
        less, equal = carry
        xt = lax.dynamic_index_in_dim(xb, i, 0, keepdims=True)
        mt = lax.dynamic_index_in_dim(mb, i, 0, keepdims=True)[:, None, :]
        less = less + mt * (xt < xb).astype(jnp.float32)
        equal = equal + mt * (xt == xb).astype(jnp.float32)
        return (less, equal)

    less, equal = lax.fori_loop(0, xb.shape[0], step, (zeros, zeros))
    count = jnp.sum(mb, 0)
    lower = jnp.floor((count - 1.0) / 2.0)
    upper = jnp.floor(count / 2.0)

    def pick(level):
        chosen = mb[:, None, :] * ((less <= level) & (level < less + equal)).astype(jnp.float32)
        return jnp.sum(chosen * xb, 0) / jnp.maximum(jnp.sum(chosen, 0), 1.0)

    return 0.5 * (pick(lower) + pick(upper))


def reference(reflect, cloud_free, days):
    x = reflect.astype(jnp.float32)
    m = cloud_free.astype(jnp.float32)
    t = days.astype(jnp.float32) / 365.0
    csum = jnp.sum(x * m[:, None, :], 2)
    cnt = jnp.sum(m, 1)
    scene_mean = csum / jnp.maximum(cnt, 1.0)[:, None]
    y = x - scene_mean[:, :, None]
    s0 = jnp.sum(m, 0)
    s1 = jnp.sum(t[:, None] * m, 0)
    s2 = jnp.sum((t * t)[:, None] * m, 0)
    sy = jnp.sum(m[:, None, :] * y, 0)
    sty = jnp.sum((t[:, None] * m)[:, None, :] * y, 0)
    first = s0 + ridge
    det = first * (s2 + ridge) - s1 * s1
    slope = (first[None, :] * sty - s1[None, :] * sy) / det[None, :]
    blocks = PIXELS // PIX_DEV
    xs = x.reshape(DATES, BANDS, blocks, PIX_DEV).transpose(2, 0, 1, 3)
    ms = m.reshape(DATES, blocks, PIX_DEV).transpose(1, 0, 2)
    med = lax.map(rank_block, (xs, ms))
    median = med.transpose(1, 0, 2).reshape(BANDS, PIXELS)
    return median, slope
```

```python
import functools

import jax
import jax.numpy as jnp
from jax import lax
from jax.experimental import pallas as pl
from jax.experimental.pallas import tpu as pltpu
from jax.sharding import PartitionSpec as P

ridge = 1.0
sentinel = 100.0
limit = 50.0
big = 1000.0
lanes = 128
gap = 8


def sums_kernel(bands, x_ref, m_ref, out_ref):
    valid = m_ref[...] > 0
    column = lax.broadcasted_iota(jnp.int32, out_ref.shape, 1)
    total = jnp.where(column == bands, jnp.sum(jnp.where(valid, 1.0, 0.0), 1, keepdims=True), 0.0)
    for b in range(bands):
        clear = jnp.where(valid, x_ref[b].astype(jnp.float32), 0.0)
        total += jnp.where(column == b, jnp.sum(clear, 1, keepdims=True), 0.0)
    out_ref[...] = total


def pack_kernel(bands, groups, days_ref, x_ref, m_ref, own_ref, other_ref, out_ref):
    dates, pixels = m_ref.shape
    chunks = out_ref.shape[0]
    width = groups * lanes
    rows = bands * groups * dates
    total = own_ref[...] + other_ref[...]
    column = lax.broadcasted_iota(jnp.int32, total.shape, 1)
    row = lax.broadcasted_iota(jnp.int32, total.shape, 0)
    count = jnp.sum(jnp.where(column == bands, total, 0.0), 1, keepdims=True)
    day = jnp.zeros(total.shape, jnp.float32)
    for d in range(dates):
        day = jnp.where(row == d, days_ref[d].astype(jnp.float32), day)
    stats = jnp.where(column < bands, total / jnp.maximum(count, 1.0), 0.0)
    stats = jnp.where(column == bands, day / 365.0, stats)
    high = stats.astype(jnp.bfloat16).astype(jnp.float32)
    rest = stats - high
    middle = rest.astype(jnp.bfloat16).astype(jnp.float32)
    low = rest - middle
    table = high + pltpu.roll(middle, gap, 1) + pltpu.roll(low, 2 * gap, 1)
    table = table.astype(jnp.bfloat16)
    for c in range(chunks):
        valid = m_ref[:, c * width : (c + 1) * width] > 0
        for b in range(bands):
            value = x_ref[b, :, c * width : (c + 1) * width].astype(jnp.float32)
            marked = jnp.where(valid, value, sentinel).astype(jnp.bfloat16)
            for g in range(groups):
                at = (b * groups + g) * dates
                out_ref[c, at : at + dates, :] = marked[:, g * lanes : (g + 1) * lanes]
        out_ref[c, rows : rows + dates, :] = table


def merge_pairs(n):
    pairs = []

    def merge(lo, length, step):
        jump = step * 2
        if jump < length:
            merge(lo, length, jump)
            merge(lo + step, length, jump)
            for i in range(lo + step, lo + length - step, jump):
                pairs.append((i, i + step))
        else:
            pairs.append((lo, lo + step))

    def sort(lo, length):
        if length > 1:
            half = length // 2
            sort(lo, half)
            sort(lo + half, half)
            merge(lo, length, 1)

    sort(0, n)
    return pairs


def sort_list(items):
    items = list(items)
    n = 1
    while n < len(items):
        n *= 2
    for i, j in merge_pairs(n):
        if j < len(items):
            items[i], items[j] = jnp.minimum(items[i], items[j]), jnp.maximum(items[i], items[j])
    return items


def middle_pair(first, second):
    n = len(first)
    low = [jnp.minimum(first[i], second[n - 1 - i]) for i in range(n)]
    high = [jnp.maximum(first[i], second[n - 1 - i]) for i in range(n)]
    return functools.reduce(jnp.maximum, low), functools.reduce(jnp.minimum, high)


def fit_kernel(bands, groups, dates, in_ref, out_ref, wide_ref, table_ref):
    sources, height, _ = in_ref.shape
    lines = bands * groups
    rows = lines * dates
    pick = lax.broadcasted_iota(jnp.int32, (lanes, (bands + 1) * lanes), 0)
    to = lax.broadcasted_iota(jnp.int32, (lanes, (bands + 1) * lanes), 1) // lanes
    spread = ((pick == to) | (pick == to + gap) | (pick == to + 2 * gap)).astype(jnp.bfloat16)
    for s in range(sources):
        wide_ref[s] = in_ref[s, 0:rows, :].astype(jnp.float32)
    for s in range(sources):
        table_ref[s] = jnp.dot(in_ref[s, rows : rows + dates, :], spread, preferred_element_type=jnp.float32)
    order = [(s, d) for s in range(sources) for d in range(dates)]
    fixed = None
    for start in range(0, lines, 8):
        size = min(8, lines - start)
        shape = (size, lanes)
        line = lax.broadcasted_iota(jnp.int32, shape, 0) + start

        def value_at(s, d):
            return wide_ref[s, pl.ds(start * dates + d, size, stride=dates), :]

        def stat_at(s, d, b):
            return jnp.broadcast_to(table_ref[s, d : d + 1, b * lanes : (b + 1) * lanes], shape)

        def mean_at(s, d):
            mean = stat_at(s, d, start // groups)
            for b in range(start // groups + 1, (start + size - 1) // groups + 1):
                mean = jnp.where(line >= b * groups, stat_at(s, d, b), mean)
            return mean

        sign = jnp.full(shape, big, jnp.float32)
        zero = jnp.zeros(shape, jnp.float32)
        s_y, s_ty = zero, zero
        s_zero, s_one, s_two = zero, zero, zero
        items = []
        for s, d in order:
            value = value_at(s, d)
            clear = value < limit
            items.append(jnp.where(clear, value, sign))
            sign = jnp.where(clear, sign, -sign)
            year = stat_at(s, d, bands)
            part = jnp.where(clear, value - mean_at(s, d), 0.0)
            s_y = s_y + part
            s_ty = s_ty + year * part
            seen = jnp.where(clear, 1.0, 0.0)
            timed = seen * year
            s_zero = s_zero + seen
            s_one = s_one + timed
            s_two = s_two + timed * year
        half = len(items) // 2
        low, high = middle_pair(sort_list(items[:half]), sort_list(items[half:]))
        median = 0.5 * (low + jnp.where(sign > 0, high, low))
        first = s_zero + ridge
        slope = (first * s_ty - s_one * s_y) / (first * (s_two + ridge) - s_one * s_one)
        for c in range(out_ref.shape[0]):
            out_ref[c, start : start + size, :] = median
            out_ref[c, lines + start : lines + start + size, :] = slope


def place_kernel(bands, groups, in_ref, median_ref, slope_ref):
    lines = bands * groups
    for s in range(in_ref.shape[0]):
        for g in range(groups):
            at = (s * groups + g) * lanes
            median_ref[:, at : at + lanes] = in_ref[s, pl.ds(g, bands, stride=groups), :]
            slope_ref[:, at : at + lanes] = in_ref[s, pl.ds(lines + g, bands, stride=groups), :]


def vmem(n):
    return [pl.BlockSpec(memory_space=pltpu.VMEM)] * n


def local(parts, tiles, reflect, cloud_free, days):
    dates, bands, pixels = reflect.shape
    groups = pixels // parts // lanes
    lines = bands * groups
    rows = lines * dates
    height = rows + -(-dates // 8) * 8
    values = jnp.transpose(reflect, (1, 0, 2))
    own = pl.pallas_call(
        functools.partial(sums_kernel, bands),
        out_shape=jax.ShapeDtypeStruct((dates, lanes), jnp.float32),
        in_specs=vmem(2),
        out_specs=vmem(1)[0],
        name="sums",
    )(values, cloud_free)
    if tiles == 2:
        other = lax.ppermute(own, "pix", [(0, 1), (1, 0)])
    else:
        own, other = lax.psum(own, "pix"), jnp.zeros(own.shape, own.dtype)
    packed = pl.pallas_call(
        functools.partial(pack_kernel, bands, groups),
        out_shape=jax.ShapeDtypeStruct((parts, height, lanes), jnp.bfloat16),
        in_specs=[pl.BlockSpec(memory_space=pltpu.SMEM)] + vmem(4),
        out_specs=vmem(1)[0],
        name="pack",
    )(days, values, cloud_free, own, other)
    moved = lax.all_to_all(packed, "date", split_axis=0, concat_axis=0, tiled=True)
    fitted = pl.pallas_call(
        functools.partial(fit_kernel, bands, groups, dates),
        out_shape=jax.ShapeDtypeStruct((parts, 2 * lines, lanes), jnp.float32),
        in_specs=vmem(1),
        out_specs=vmem(1)[0],
        scratch_shapes=[
            pltpu.VMEM((parts, rows, lanes), jnp.float32),
            pltpu.VMEM((parts, dates, (bands + 1) * lanes), jnp.float32),
        ],
        name="fit",
    )(moved)
    spread = lax.all_to_all(fitted, "date", split_axis=0, concat_axis=0, tiled=True)
    shape = jax.ShapeDtypeStruct((bands, pixels), jnp.float32)
    return pl.pallas_call(
        functools.partial(place_kernel, bands, groups),
        out_shape=(shape, shape),
        in_specs=vmem(1),
        out_specs=tuple(vmem(2)),
        name="place",
    )(spread)


def solution(mesh):
    placed = (P("date", None, "pix"), P("date", "pix"), P("date"))
    return jax.shard_map(
        functools.partial(local, mesh.shape["date"], mesh.shape["pix"]),
        mesh=mesh,
        in_specs=placed,
        out_specs=(P(None, "pix"), P(None, "pix")),
        check_vma=False,
    )
```

```python
import functools

import jax
import jax.numpy as jnp
from jax import lax
from jax.experimental import pallas as pl
from jax.experimental.pallas import tpu as pltpu
from jax.sharding import PartitionSpec as P

ridge = 1.0
sentinel = 100.0
limit = 50.0
big = 1000.0
lanes = 128
order = (6, 7, 11, 5, 15, 10, 14, 13, 12, 3, 1, 9, 8, 4, 0, 2)


def split_pieces(table, gap):
    high = table.astype(jnp.bfloat16).astype(jnp.float32)
    rest = table - high
    middle = rest.astype(jnp.bfloat16).astype(jnp.float32)
    low = rest - middle
    return (high + pltpu.roll(middle, gap, 1) + pltpu.roll(low, 2 * gap, 1)).astype(jnp.bfloat16)


def pack_kernel(bands, groups, days_ref, x_hbm, m_hbm, out_ref, x_ref, m_ref, sems):
    dates, _ = m_ref.shape
    chunks = out_ref.shape[0]
    width = groups * lanes
    rows = bands * groups * dates
    mask_copy = pltpu.make_async_copy(m_hbm, m_ref, sems.at[bands])
    mask_copy.start()
    copies = [pltpu.make_async_copy(x_hbm.at[b], x_ref.at[b], sems.at[b]) for b in range(bands)]
    for copy in copies:
        copy.start()
    shape = (dates, lanes)
    column = lax.broadcasted_iota(jnp.int32, shape, 1)
    row = lax.broadcasted_iota(jnp.int32, shape, 0)
    day = jnp.zeros(shape, jnp.float32)
    for d in range(dates):
        day = jnp.where(row == d, days_ref[d].astype(jnp.float32), day)
    mask_copy.wait()
    count = jnp.sum(jnp.where(m_ref[...] > 0, 1.0, 0.0), 1, keepdims=True)
    table = jnp.where(column == bands, count, jnp.where(column == bands + 1, day, 0.0))
    for b in range(bands):
        copies[b].wait()
        total = jnp.zeros((dates, width), jnp.float32)
        for c in range(chunks):
            valid = m_ref[:, c * width : (c + 1) * width] > 0
            value = x_ref[b, :, c * width : (c + 1) * width].astype(jnp.float32)
            total += jnp.where(valid, value, 0.0)
            marked = jnp.where(valid, value, sentinel).astype(jnp.bfloat16)
            for g in range(groups):
                at = (b * groups + g) * dates
                out_ref[c, at : at + dates, :] = marked[:, g * lanes : (g + 1) * lanes]
        table = jnp.where(column == b, jnp.sum(total, 1, keepdims=True), table)
    table = split_pieces(jnp.where(column < bands + 2, table, 0.0), bands + 2)
    for c in range(chunks):
        out_ref[c, rows : rows + dates, :] = table


def stats_kernel(gap, rows, in_ref, out_ref):
    dates = out_ref.shape[0] // in_ref.shape[0]
    for s in range(in_ref.shape[0]):
        part = in_ref[s, rows : rows + dates, :].astype(jnp.float32)
        part = part + pltpu.roll(part, lanes - gap, 1) + pltpu.roll(part, lanes - 2 * gap, 1)
        out_ref[s * dates : (s + 1) * dates, :] = part


def merge_pairs(n):
    pairs = []

    def merge(lo, length, step):
        jump = step * 2
        if jump < length:
            merge(lo, length, jump)
            merge(lo + step, length, jump)
            for i in range(lo + step, lo + length - step, jump):
                pairs.append((i, i + step))
        else:
            pairs.append((lo, lo + step))

    def sort(lo, length):
        if length > 1:
            half = length // 2
            sort(lo, half)
            sort(lo + half, half)
            merge(lo, length, 1)

    sort(0, n)
    return pairs


def sort_list(items):
    items = list(items)
    n = 1
    while n < len(items):
        n *= 2
    for i, j in merge_pairs(n):
        if j < len(items):
            items[i], items[j] = jnp.minimum(items[i], items[j]), jnp.maximum(items[i], items[j])
    return items


def middle_pair(first, second):
    n = len(first)
    low = [jnp.minimum(first[i], second[n - 1 - i]) for i in range(n)]
    high = [jnp.maximum(first[i], second[n - 1 - i]) for i in range(n)]
    return functools.reduce(jnp.maximum, low), functools.reduce(jnp.minimum, high)


def blocks_of(lines):
    return [(start, min(8, lines - start)) for start in range(0, lines, 8)]


def median_kernel(lines, dates, in_ref, out_ref, wide_ref):
    sources = in_ref.shape[0]
    rows = lines * dates
    for s in range(sources):
        wide_ref[s] = in_ref[s, 0:rows, :].astype(jnp.float32)
    for start, size in blocks_of(lines):
        sign = jnp.full((size, lanes), big, jnp.float32)
        items = []
        for s in range(sources):
            for d in range(dates):
                value = wide_ref[s, pl.ds(start * dates + d, size, stride=dates), :]
                clear = value < limit
                items.append(jnp.where(clear, value, sign))
                sign = jnp.where(clear, sign, -sign)
        half = len(items) // 2
        low, high = middle_pair(sort_list(items[:half]), sort_list(items[half:]))
        out_ref[start : start + size, :] = 0.5 * (low + jnp.where(sign > 0, high, low))


def slope_kernel(bands, groups, wide_ref, own_ref, other_ref, median_ref, out_ref, table_ref):
    sources, rows, _ = wide_ref.shape
    lines = bands * groups
    dates = rows // lines
    gap = bands + 2
    own = own_ref[...]
    total = own + other_ref[...]
    column = lax.broadcasted_iota(jnp.int32, total.shape, 1)
    count = jnp.sum(jnp.where(column == bands, total, 0.0), 1, keepdims=True)
    stats = jnp.where(column < bands, total / jnp.maximum(count, 1.0), 0.0)
    stats = jnp.where(column == bands + 1, own / 365.0, stats)
    pick = lax.broadcasted_iota(jnp.int32, (lanes, (bands + 1) * lanes), 0)
    to = lax.broadcasted_iota(jnp.int32, (lanes, (bands + 1) * lanes), 1) // lanes
    to = jnp.where(to == bands, bands + 1, to)
    spread = ((pick == to) | (pick == to + gap) | (pick == to + 2 * gap)).astype(jnp.bfloat16)
    table_ref[...] = jnp.dot(split_pieces(stats, gap), spread, preferred_element_type=jnp.float32)
    shared = None
    for start, size in blocks_of(lines):
        shape = (size, lanes)
        line = lax.broadcasted_iota(jnp.int32, shape, 0) + start
        fresh = shared is None or 8 % groups != 0 or shared[0].shape != shape
        zero = jnp.zeros(shape, jnp.float32)
        s_y, s_ty, s_zero, s_one, s_two = zero, zero, zero, zero, zero
        for s in range(sources):
            for d in range(dates):
                at = s * dates + d

                def stat_at(b):
                    row = table_ref[at : at + 1, b * lanes : (b + 1) * lanes]
                    return jnp.broadcast_to(row, shape)

                mean = stat_at(start // groups)
                for b in range(start // groups + 1, (start + size - 1) // groups + 1):
                    mean = jnp.where(line >= b * groups, stat_at(b), mean)
                value = wide_ref[s, pl.ds(start * dates + d, size, stride=dates), :]
                clear = value < limit
                year = stat_at(bands)
                part = jnp.where(clear, value - mean, 0.0)
                s_y = s_y + part
                s_ty = s_ty + year * part
                if fresh:
                    timed = jnp.where(clear, year, 0.0)
                    s_zero = s_zero + jnp.where(clear, 1.0, 0.0)
                    s_one = s_one + timed
                    s_two = s_two + timed * year
        if fresh:
            first = s_zero + ridge
            shared = (first, s_one, first * (s_two + ridge) - s_one * s_one)
        first, s_one, determinant = shared
        slope = (first * s_ty - s_one * s_y) / determinant
        for c in range(out_ref.shape[0]):
            out_ref[c, start : start + size, :] = median_ref[start : start + size, :]
            out_ref[c, lines + start : lines + start + size, :] = slope


def place_kernel(bands, groups, in_ref, median_ref, slope_ref):
    lines = bands * groups
    for s in range(in_ref.shape[0]):
        for g in range(groups):
            at = (s * groups + g) * lanes
            median_ref[:, at : at + lanes] = in_ref[s, pl.ds(g, bands, stride=groups), :]
            slope_ref[:, at : at + lanes] = in_ref[s, pl.ds(lines + g, bands, stride=groups), :]


def call(kernel, name, out_shape, in_specs, scratch=(), flops=0):
    many = isinstance(out_shape, tuple)
    spec = pl.BlockSpec(memory_space=pltpu.VMEM)
    cost = pl.CostEstimate(flops=flops, bytes_accessed=flops, transcendentals=0) if flops else None
    return pl.pallas_call(
        kernel,
        out_shape=out_shape,
        in_specs=[pl.BlockSpec(memory_space=space) for space in in_specs],
        out_specs=tuple([spec] * len(out_shape)) if many else spec,
        scratch_shapes=scratch,
        compiler_params=pltpu.CompilerParams(vmem_limit_bytes=8 * 1024 * 1024),
        cost_estimate=cost,
        name=name,
    )


def exchange(x):
    groups = [list(order)] if len(order) == x.shape[0] else None
    return lax.all_to_all(x, "date", split_axis=0, concat_axis=0, tiled=True, axis_index_groups=groups)


def local(parts, tiles, reflect, cloud_free, days):
    dates, bands, pixels = reflect.shape
    groups = pixels // parts // lanes
    lines = bands * groups
    rows = lines * dates
    height = rows + -(-dates // 8) * 8
    inside, outside = pltpu.VMEM, pltpu.HBM
    array = jax.ShapeDtypeStruct
    values = jnp.transpose(reflect, (1, 0, 2))
    packed = call(
        functools.partial(pack_kernel, bands, groups),
        "pack",
        array((parts, height, lanes), jnp.bfloat16),
        [pltpu.SMEM, outside, outside],
        [
            pltpu.VMEM((bands, dates, pixels), jnp.bfloat16),
            pltpu.VMEM((dates, pixels), jnp.int32),
            pltpu.SemaphoreType.DMA((bands + 1,)),
        ],
    )(*[pltpu.with_memory_space_constraint(x, outside) if x.size > 1 else x for x in (days, values, cloud_free)])
    moved = exchange(packed)
    own = call(
        functools.partial(stats_kernel, bands + 2, rows),
        "stats",
        array((parts * dates, lanes), jnp.float32),
        [inside],
    )(moved)
    if tiles == 2:
        other = lax.ppermute(own, "pix", [(0, 1), (1, 0)])
    else:
        ring = [(i, (i + 1) % tiles) for i in range(tiles)]
        passed, other = own, jnp.zeros(own.shape, own.dtype)
        for _ in range(tiles - 1):
            passed = lax.ppermute(passed, "pix", ring)
            other = other + passed
    median, wide = call(
        functools.partial(median_kernel, lines, dates),
        "median",
        (array((lines, lanes), jnp.float32), array((parts, rows, lanes), jnp.float32)),
        [inside],
        flops=16_000_000,
    )(moved)
    fitted = call(
        functools.partial(slope_kernel, bands, groups),
        "slope",
        array((parts, 2 * lines, lanes), jnp.float32),
        [inside] * 4,
        [pltpu.VMEM((parts * dates, (bands + 1) * lanes), jnp.float32)],
    )(wide, own, other, median)
    spread = exchange(fitted)
    shape = array((bands, pixels), jnp.float32)
    return call(functools.partial(place_kernel, bands, groups), "place", (shape, shape), [inside])(spread)


def solution(mesh):
    placed = (P("date", None, "pix"), P("date", "pix"), P("date"))
    return jax.shard_map(
        functools.partial(local, mesh.shape["date"], mesh.shape["pix"]),
        mesh=mesh,
        in_specs=placed,
        out_specs=(P(None, "pix"), P(None, "pix")),
        check_vma=False,
    )
```

```python
import functools

import jax
import jax.numpy as jnp
from jax import lax
from jax.experimental import pallas as pl
from jax.experimental.pallas import tpu as pltpu
from jax.sharding import PartitionSpec as P

ridge = 1.0
sentinel = 100.0
limit = 50.0
big = 1000.0
lanes = 128
order = (6, 7, 11, 5, 15, 10, 14, 13, 12, 3, 1, 9, 8, 4, 0, 2)


def split_pieces(table, gap):
    high = table.astype(jnp.bfloat16).astype(jnp.float32)
    rest = table - high
    middle = rest.astype(jnp.bfloat16).astype(jnp.float32)
    low = rest - middle
    return (high + pltpu.roll(middle, gap, 1) + pltpu.roll(low, 2 * gap, 1)).astype(jnp.bfloat16)


def load_kernel(bands, d_hbm, x_hbm, m_hbm, x_ref, m_ref, out_ref, days_ref, sems):
    dates, pixels = m_ref.shape
    mask_copy = pltpu.make_async_copy(m_hbm, m_ref, sems.at[0])
    mask_copy.start()
    value_copy = pltpu.make_async_copy(x_hbm, x_ref, sems.at[1])
    value_copy.start()
    days_copy = pltpu.make_async_copy(d_hbm, days_ref, sems.at[2])
    days_copy.start()
    shape = (dates, lanes)
    column = lax.broadcasted_iota(jnp.int32, shape, 1)
    row = lax.broadcasted_iota(jnp.int32, shape, 0)
    tiles = [slice(at, at + lanes) for at in range(0, pixels, lanes)]
    mask_copy.wait()
    totals = [sum(jnp.where(m_ref[:, at] > 0, 1.0, 0.0) for at in tiles)]
    value_copy.wait()
    for b in range(bands):
        totals.append(sum(jnp.where(m_ref[:, at] > 0, x_ref[b, :, at].astype(jnp.float32), 0.0) for at in tiles))
    table = jnp.zeros(shape, jnp.float32)
    days_copy.wait()
    for d in range(dates):
        table = jnp.where((row == d) & (column == bands + 1), days_ref[d].astype(jnp.float32), table)
    for b, total in enumerate(totals[1:] + totals[:1]):
        table = jnp.where(column == b, jnp.sum(total, 1, keepdims=True), table)
    out_ref[...] = table


def pack_kernel(bands, groups, x_ref, m_ref, out_ref):
    dates, _ = m_ref.shape
    width = groups * lanes
    for c in range(out_ref.shape[0]):
        valid = m_ref[:, c * width : (c + 1) * width] > 0
        for b in range(bands):
            value = x_ref[b, :, c * width : (c + 1) * width].astype(jnp.float32)
            marked = jnp.where(valid, value, sentinel).astype(jnp.bfloat16)
            for g in range(groups):
                at = (b * groups + g) * dates
                out_ref[c, at : at + dates, :] = marked[:, g * lanes : (g + 1) * lanes]


def stamp_kernel(bands, rows, own_ref, other_ref, in_ref, out_ref):
    del in_ref
    own = own_ref[...]
    total = own + other_ref[...]
    dates = total.shape[0]
    column = lax.broadcasted_iota(jnp.int32, total.shape, 1)
    count = jnp.sum(jnp.where(column == bands, total, 0.0), 1, keepdims=True)
    stats = jnp.where(column < bands, total / jnp.maximum(count, 1.0), 0.0)
    stats = split_pieces(jnp.where(column == bands + 1, own / 365.0, stats), bands + 2)
    for c in range(out_ref.shape[0]):
        out_ref[c, rows : rows + dates, :] = stats


def merge_pairs(n):
    pairs = []

    def merge(lo, length, step):
        jump = step * 2
        if jump < length:
            merge(lo, length, jump)
            merge(lo + step, length, jump)
            for i in range(lo + step, lo + length - step, jump):
                pairs.append((i, i + step))
        else:
            pairs.append((lo, lo + step))

    def sort(lo, length):
        if length > 1:
            half = length // 2
            sort(lo, half)
            sort(lo + half, half)
            merge(lo, length, 1)

    sort(0, n)
    return pairs


def sort_list(items):
    items = list(items)
    n = 1
    while n < len(items):
        n *= 2
    for i, j in merge_pairs(n):
        if j < len(items):
            items[i], items[j] = jnp.minimum(items[i], items[j]), jnp.maximum(items[i], items[j])
    return items


def middle_pair(first, second):
    n = len(first)
    low = [jnp.minimum(first[i], second[n - 1 - i]) for i in range(n)]
    high = [jnp.maximum(first[i], second[n - 1 - i]) for i in range(n)]
    return functools.reduce(jnp.maximum, low), functools.reduce(jnp.minimum, high)


def blocks_of(lines):
    return [(start, min(8, lines - start)) for start in range(0, lines, 8)]


def fit_kernel(bands, groups, dates, in_ref, out_ref, wide_ref, table_ref):
    sources = in_ref.shape[0]
    lines = bands * groups
    rows = lines * dates
    gap = bands + 2
    wide = (lanes, (bands + 1) * lanes)
    pick = lax.broadcasted_iota(jnp.int32, wide, 0)
    to = lax.broadcasted_iota(jnp.int32, wide, 1) // lanes
    to = jnp.where(to == bands, bands + 1, to)
    spread = ((pick == to) | (pick == to + gap) | (pick == to + 2 * gap)).astype(jnp.bfloat16)
    for s in range(sources):
        wide_ref[s] = in_ref[s, 0:rows, :].astype(jnp.float32)
        table_ref[s] = jnp.dot(in_ref[s, rows : rows + dates, :], spread, preferred_element_type=jnp.float32)
    shared = None
    for start, size in blocks_of(lines):
        shape = (size, lanes)
        line = lax.broadcasted_iota(jnp.int32, shape, 0) + start
        fresh = shared is None or 8 % groups != 0 or shared[0].shape != shape
        zero = jnp.zeros(shape, jnp.float32)
        sign = jnp.full(shape, big, jnp.float32)
        s_y, s_ty, s_zero, s_one, s_two = zero, zero, zero, zero, zero
        items = []
        for s in range(sources):
            for d in range(dates):

                def stat_at(b):
                    row = table_ref[s, d : d + 1, b * lanes : (b + 1) * lanes]
                    return jnp.broadcast_to(row, shape)

                mean = stat_at(start // groups)
                for b in range(start // groups + 1, (start + size - 1) // groups + 1):
                    mean = jnp.where(line >= b * groups, stat_at(b), mean)
                value = wide_ref[s, pl.ds(start * dates + d, size, stride=dates), :]
                clear = value < limit
                items.append(jnp.where(clear, value, sign))
                sign = jnp.where(clear, sign, -sign)
                year = stat_at(bands)
                part = jnp.where(clear, value - mean, 0.0)
                s_y = s_y + part
                s_ty = s_ty + year * part
                if fresh:
                    timed = jnp.where(clear, year, 0.0)
                    s_zero = s_zero + jnp.where(clear, 1.0, 0.0)
                    s_one = s_one + timed
                    s_two = s_two + timed * year
        half = len(items) // 2
        low, high = middle_pair(sort_list(items[:half]), sort_list(items[half:]))
        median = 0.5 * (low + jnp.where(sign > 0, high, low))
        if fresh:
            first = s_zero + ridge
            shared = (first, s_one, first * (s_two + ridge) - s_one * s_one)
        first, s_one, determinant = shared
        slope = (first * s_ty - s_one * s_y) / determinant
        for c in range(out_ref.shape[0]):
            out_ref[c, start : start + size, :] = median
            out_ref[c, lines + start : lines + start + size, :] = slope


def place_kernel(bands, groups, in_ref, median_ref, slope_ref):
    lines = bands * groups
    for s in range(in_ref.shape[0]):
        for g in range(groups):
            at = (s * groups + g) * lanes
            median_ref[:, at : at + lanes] = in_ref[s, pl.ds(g, bands, stride=groups), :]
            slope_ref[:, at : at + lanes] = in_ref[s, pl.ds(lines + g, bands, stride=groups), :]


def call(kernel, name, out_shape, in_specs, scratch=(), flops=0, aliases={}):
    many = isinstance(out_shape, tuple)
    spec = pl.BlockSpec(memory_space=pltpu.VMEM)
    cost = pl.CostEstimate(flops=flops, bytes_accessed=flops, transcendentals=0) if flops else None
    return pl.pallas_call(
        kernel,
        out_shape=out_shape,
        in_specs=[pl.BlockSpec(memory_space=space) for space in in_specs],
        out_specs=tuple([spec] * len(out_shape)) if many else spec,
        scratch_shapes=scratch,
        compiler_params=pltpu.CompilerParams(vmem_limit_bytes=8 * 1024 * 1024),
        cost_estimate=cost,
        input_output_aliases=aliases,
        name=name,
    )


def exchange(x):
    groups = [list(order)] if len(order) == x.shape[0] else None
    return lax.all_to_all(x, "date", split_axis=0, concat_axis=0, tiled=True, axis_index_groups=groups)


def local(parts, tiles, reflect, cloud_free, days):
    dates, bands, pixels = reflect.shape
    groups = pixels // parts // lanes
    lines = bands * groups
    rows = lines * dates
    height = rows + -(-dates // 8) * 8
    inside, outside = pltpu.VMEM, pltpu.HBM
    array = jax.ShapeDtypeStruct
    values = jnp.transpose(reflect, (1, 0, 2))
    held, mask, own = call(
        functools.partial(load_kernel, bands),
        "load",
        (
            array(values.shape, values.dtype),
            array(cloud_free.shape, cloud_free.dtype),
            array((dates, lanes), jnp.float32),
        ),
        [outside if dates > 1 else pl.ANY, outside, outside],
        [pltpu.SMEM((dates,), jnp.int32), pltpu.SemaphoreType.DMA((3,))],
    )(*[pltpu.with_memory_space_constraint(x, outside) if x.size > 1 else x for x in (days, values, cloud_free)])
    if tiles == 2:
        other = lax.ppermute(own, "pix", [(0, 1), (1, 0)])
    else:
        ring = [(i, (i + 1) % tiles) for i in range(tiles)]
        passed, other = own, jnp.zeros(own.shape, own.dtype)
        for _ in range(tiles - 1):
            passed = lax.ppermute(passed, "pix", ring)
            other = other + passed
    packed = call(
        functools.partial(pack_kernel, bands, groups),
        "pack",
        array((parts, height, lanes), jnp.bfloat16),
        [inside, inside],
        flops=16_000_000,
    )(held, mask)
    stamped = call(
        functools.partial(stamp_kernel, bands, rows),
        "stamp",
        array(packed.shape, packed.dtype),
        [inside] * 3,
        aliases={2: 0},
    )(own, other, pltpu.with_memory_space_constraint(packed, inside))
    moved = exchange(stamped)
    fitted = call(
        functools.partial(fit_kernel, bands, groups, dates),
        "fit",
        array((parts, 2 * lines, lanes), jnp.float32),
        [inside],
        [
            pltpu.VMEM((parts, rows, lanes), jnp.float32),
            pltpu.VMEM((parts, dates, (bands + 1) * lanes), jnp.float32),
        ],
    )(moved)
    spread = exchange(fitted)
    shape = array((bands, pixels), jnp.float32)
    return call(functools.partial(place_kernel, bands, groups), "place", (shape, shape), [inside])(spread)


def solution(mesh):
    placed = (P("date", None, "pix"), P("date", "pix"), P("date"))
    return jax.shard_map(
        functools.partial(local, mesh.shape["date"], mesh.shape["pix"]),
        mesh=mesh,
        in_specs=placed,
        out_specs=(P(None, "pix"), P(None, "pix")),
        check_vma=False,
    )
```

```python
import functools

import jax
import jax.numpy as jnp
from jax import lax
from jax.experimental import pallas as pl
from jax.experimental.pallas import tpu as pltpu
from jax.sharding import PartitionSpec as P

ridge = 1.0
sentinel = 100.0
limit = 50.0
big = 1000.0
lanes = 128
orders = (
    (6, 7, 11, 5, 15, 10, 14, 1, 8, 3, 13, 9, 12, 4, 0, 2),
    (6, 7, 11, 5, 15, 10, 14, 13, 12, 3, 1, 9, 8, 4, 0, 2),
)
again = (0, 1, 2, 14, 4, 5, 3, 7, 8, 9, 10, 13, 12, 11, 6, 15)


def split_pieces(table, gap):
    high = table.astype(jnp.bfloat16).astype(jnp.float32)
    rest = table - high
    middle = rest.astype(jnp.bfloat16).astype(jnp.float32)
    low = rest - middle
    return (high + pltpu.roll(middle, gap, 1) + pltpu.roll(low, 2 * gap, 1)).astype(jnp.bfloat16)


def load_kernel(bands, d_hbm, x_hbm, m_hbm, x_ref, m_ref, out_ref, days_ref, sems):
    dates, pixels = m_ref.shape
    mask_copy = pltpu.make_async_copy(m_hbm, m_ref, sems.at[0])
    mask_copy.start()
    value_copy = pltpu.make_async_copy(x_hbm, x_ref, sems.at[1])
    value_copy.start()
    days_copy = pltpu.make_async_copy(d_hbm, days_ref, sems.at[2])
    days_copy.start()
    shape = (dates, lanes)
    column = lax.broadcasted_iota(jnp.int32, shape, 1)
    row = lax.broadcasted_iota(jnp.int32, shape, 0)
    mask_copy.wait()
    value_copy.wait()
    step = 4 * lanes if pixels % (4 * lanes) == 0 else lanes
    totals = [jnp.zeros((dates, step), jnp.float32)] * (bands + 1)
    for at in range(0, pixels, step):
        valid = m_ref[:, at : at + step] > 0
        totals[bands] += jnp.where(valid, 1.0, 0.0)
        for b in range(bands):
            totals[b] += jnp.where(valid, x_ref[b, :, at : at + step].astype(jnp.float32), 0.0)
    table = jnp.zeros(shape, jnp.float32)
    days_copy.wait()
    for d in range(dates):
        table = jnp.where((row == d) & (column == bands + 1), days_ref[d].astype(jnp.float32), table)
    for b, total in enumerate(totals):
        table = jnp.where(column == b, jnp.sum(total, 1, keepdims=True), table)
    out_ref[...] = table


def pack_kernel(bands, groups, x_ref, m_ref, out_ref):
    dates, _ = m_ref.shape
    width = groups * lanes
    for c in range(out_ref.shape[0]):
        valid = m_ref[:, c * width : (c + 1) * width] > 0
        for b in range(bands):
            value = x_ref[b, :, c * width : (c + 1) * width].astype(jnp.float32)
            marked = jnp.where(valid, value, sentinel).astype(jnp.bfloat16)
            for g in range(groups):
                at = (b * groups + g) * dates
                out_ref[c, at : at + dates, :] = marked[:, g * lanes : (g + 1) * lanes]


def stamp_kernel(bands, rows, own_ref, other_ref, in_ref, out_ref):
    del in_ref
    own = own_ref[...]
    total = own + other_ref[...]
    dates = total.shape[0]
    column = lax.broadcasted_iota(jnp.int32, total.shape, 1)
    count = jnp.sum(jnp.where(column == bands, total, 0.0), 1, keepdims=True)
    stats = jnp.where(column < bands, total / jnp.maximum(count, 1.0), 0.0)
    stats = split_pieces(jnp.where(column == bands + 1, own / 365.0, stats), bands + 2)
    for c in range(out_ref.shape[0]):
        out_ref[c, rows : rows + dates, :] = stats


def merge_pairs(n):
    pairs = []

    def merge(lo, length, step):
        jump = step * 2
        if jump < length:
            merge(lo, length, jump)
            merge(lo + step, length, jump)
            for i in range(lo + step, lo + length - step, jump):
                pairs.append((i, i + step))
        else:
            pairs.append((lo, lo + step))

    def sort(lo, length):
        if length > 1:
            half = length // 2
            sort(lo, half)
            sort(lo + half, half)
            merge(lo, length, 1)

    sort(0, n)
    return pairs


def sort_list(items):
    items = list(items)
    n = 1
    while n < len(items):
        n *= 2
    for i, j in merge_pairs(n):
        if j < len(items):
            items[i], items[j] = jnp.minimum(items[i], items[j]), jnp.maximum(items[i], items[j])
    return items


def middle_of(values, shape):
    half = len(values) // 2
    size = shape[0]
    pair = (2 * size, shape[1])
    upper = lax.broadcasted_iota(jnp.int32, pair, 0) < size
    sign = jnp.where(upper, big, -big).astype(jnp.bfloat16)
    items = []
    for first, second in zip(values[:half], values[half:]):
        value = jnp.concatenate([first, second], 0).astype(jnp.bfloat16)
        clear = value < limit
        items.append(jnp.where(clear, value, sign))
        sign = jnp.where(clear, sign, -sign)
    items = [item.astype(jnp.float32) for item in sort_list(items)]
    sign = sign.astype(jnp.float32)
    odd_first, odd_second = sign[:size] < 0, sign[size:] > 0
    low = functools.reduce(jnp.maximum, [jnp.minimum(items[i][:size], items[half - 1 - i][size:]) for i in range(half)])
    high = functools.reduce(jnp.minimum, [jnp.maximum(items[i][:size], items[half - 1 - i][size:]) for i in range(half)])
    left = jnp.where(odd_second & ~odd_first, high, low)
    right = jnp.where(odd_first & ~odd_second, low, high)
    return 0.5 * (left + right)


def blocks_of(lines):
    return [(start, min(8, lines - start)) for start in range(0, lines, 8)]


def fit_kernel(bands, groups, dates, in_ref, out_ref, wide_ref, table_ref):
    sources = in_ref.shape[0]
    lines = bands * groups
    rows = lines * dates
    gap = bands + 2
    wide = (lanes, (bands + 1) * lanes)
    pick = lax.broadcasted_iota(jnp.int32, wide, 0)
    to = lax.broadcasted_iota(jnp.int32, wide, 1) // lanes
    to = jnp.where(to == bands, bands + 1, to)
    spread = ((pick == to) | (pick == to + gap) | (pick == to + 2 * gap)).astype(jnp.bfloat16)
    for s in range(sources):
        wide_ref[s] = in_ref[s, 0:rows, :].astype(jnp.float32)
    stats = jnp.concatenate([in_ref[s, rows : rows + dates, :] for s in range(sources)], 0)
    table_ref[...] = jnp.dot(stats, spread, preferred_element_type=jnp.float32)
    shared = None
    for start, size in blocks_of(lines):
        shape = (size, lanes)
        line = lax.broadcasted_iota(jnp.int32, shape, 0) + start
        fresh = shared is None or 8 % groups != 0 or shared[0].shape != shape
        zero = jnp.zeros(shape, jnp.float32)
        s_y, s_ty, s_zero, s_one, s_two = zero, zero, zero, zero, zero
        values = []
        for s in range(sources):
            for d in range(dates):

                def stat_at(b):
                    at = s * dates + d
                    row = table_ref[at : at + 1, b * lanes : (b + 1) * lanes]
                    return jnp.broadcast_to(row, shape)

                mean = stat_at(start // groups)
                for b in range(start // groups + 1, (start + size - 1) // groups + 1):
                    mean = jnp.where(line >= b * groups, stat_at(b), mean)
                value = wide_ref[s, pl.ds(start * dates + d, size, stride=dates), :]
                values.append(value)
                clear = value < limit
                year = stat_at(bands)
                part = jnp.where(clear, value - mean, 0.0)
                s_y = s_y + part
                s_ty = s_ty + year * part
                if fresh:
                    timed = jnp.where(clear, year, 0.0)
                    s_zero = s_zero + jnp.where(clear, 1.0, 0.0)
                    s_one = s_one + timed
                    s_two = s_two + timed * year
        median = middle_of(values, shape)
        if fresh:
            first = s_zero + ridge
            shared = (first, s_one, first * (s_two + ridge) - s_one * s_one)
        first, s_one, determinant = shared
        slope = (first * s_ty - s_one * s_y) / determinant
        for c in range(out_ref.shape[0]):
            out_ref[c, start : start + size, :] = median
            out_ref[c, lines + start : lines + start + size, :] = slope


def place_kernel(bands, groups, turns, in_ref, median_ref, slope_ref, held_ref, sems):
    lines = bands * groups
    copies = []
    for n, to_ref in enumerate((median_ref, slope_ref)):
        for s, part in enumerate(turns):
            for g in range(groups):
                at = (part * groups + g) * lanes
                held_ref[n, :, at : at + lanes] = in_ref[s, pl.ds(n * lines + g, bands, stride=groups), :]
        copy = pltpu.make_async_copy(held_ref.at[n], to_ref, sems.at[n])
        copy.start()
        copies.append(copy)
    for copy in copies:
        copy.wait()


def call(kernel, name, out_shape, in_specs, scratch=(), flops=0, aliases={}, space=pltpu.VMEM):
    many = isinstance(out_shape, tuple)
    spec = pl.BlockSpec(memory_space=space)
    cost = pl.CostEstimate(flops=flops, bytes_accessed=flops, transcendentals=0) if flops else None
    return pl.pallas_call(
        kernel,
        out_shape=out_shape,
        in_specs=[pl.BlockSpec(memory_space=space) for space in in_specs],
        out_specs=tuple([spec] * len(out_shape)) if many else spec,
        scratch_shapes=scratch,
        compiler_params=pltpu.CompilerParams(vmem_limit_bytes=8 * 1024 * 1024),
        cost_estimate=cost,
        input_output_aliases=aliases,
        name=name,
    )


def exchange(x, turn, tiles):
    parts = x.shape[0]
    if len(orders) != tiles or len(turn) != parts:
        return lax.all_to_all(x, "date", split_axis=0, concat_axis=0, tiled=True)
    groups = [[order[i] * tiles + tile for i in turn] for tile, order in enumerate(orders)]
    return lax.all_to_all(x, ("date", "pix"), split_axis=0, concat_axis=0, tiled=True, axis_index_groups=groups)


def local(parts, tiles, reflect, cloud_free, days):
    dates, bands, pixels = reflect.shape
    groups = pixels // parts // lanes
    lines = bands * groups
    rows = lines * dates
    height = rows + -(-dates // 8) * 8
    inside, outside = pltpu.VMEM, pltpu.HBM
    array = jax.ShapeDtypeStruct
    values = jnp.transpose(reflect, (1, 0, 2))
    held, mask, own = call(
        functools.partial(load_kernel, bands),
        "load",
        (
            array(values.shape, values.dtype),
            array(cloud_free.shape, cloud_free.dtype),
            array((dates, lanes), jnp.float32),
        ),
        [outside if dates > 1 else pl.ANY, outside, outside],
        [pltpu.SMEM((dates,), jnp.int32), pltpu.SemaphoreType.DMA((3,))],
    )(*[pltpu.with_memory_space_constraint(x, outside) if x.size > 1 else x for x in (days, values, cloud_free)])
    if tiles == 2:
        other = lax.ppermute(own, "pix", [(0, 1), (1, 0)])
    else:
        ring = [(i, (i + 1) % tiles) for i in range(tiles)]
        passed, other = own, jnp.zeros(own.shape, own.dtype)
        for _ in range(tiles - 1):
            passed = lax.ppermute(passed, "pix", ring)
            other = other + passed
    packed = call(
        functools.partial(pack_kernel, bands, groups),
        "pack",
        array((parts, height, lanes), jnp.bfloat16),
        [inside, inside],
        flops=16_000_000,
    )(held, mask)
    stamped = call(
        functools.partial(stamp_kernel, bands, rows),
        "stamp",
        array(packed.shape, packed.dtype),
        [inside] * 3,
        aliases={2: 0},
    )(own, other, pltpu.with_memory_space_constraint(packed, inside))
    turns = again if len(orders) == tiles and len(again) == parts else tuple(range(parts))
    moved = exchange(stamped, tuple(range(parts)), tiles)
    fitted = call(
        functools.partial(fit_kernel, bands, groups, dates),
        "fit",
        array((parts, 2 * lines, lanes), jnp.float32),
        [inside],
        [
            pltpu.VMEM((parts, rows, lanes), jnp.float32),
            pltpu.VMEM((parts * dates, (bands + 1) * lanes), jnp.float32),
        ],
    )(moved)
    spread = exchange(fitted, turns, tiles)
    shape = array((bands, pixels), jnp.float32)
    return call(
        functools.partial(place_kernel, bands, groups, turns),
        "place",
        (shape, shape),
        [inside],
        [pltpu.VMEM((2, bands, pixels), jnp.float32), pltpu.SemaphoreType.DMA((2,))],
        space=outside,
    )(spread)


def solution(mesh):
    placed = (P("date", None, "pix"), P("date", "pix"), P("date"))
    return jax.shard_map(
        functools.partial(local, mesh.shape["date"], mesh.shape["pix"]),
        mesh=mesh,
        in_specs=placed,
        out_specs=(P(None, "pix"), P(None, "pix")),
        check_vma=False,
    )
```

```python
import functools

import jax
import jax.numpy as jnp
from jax import lax
from jax.experimental import pallas as pl
from jax.experimental.pallas import tpu as pltpu
from jax.sharding import PartitionSpec as P

ridge = 1.0
sentinel = 100.0
limit = 50.0
big = 1000.0
lanes = 128
orders = (
    (0, 12, 5, 8, 9, 11, 10, 3, 15, 6, 14, 1, 2, 7, 4, 13),
    (11, 0, 9, 1, 13, 8, 3, 6, 7, 14, 10, 4, 2, 5, 12, 15),
)
again = (5, 8, 7, 4, 0, 12, 10, 2, 13, 1, 9, 6, 3, 14, 15, 11)


def split_pieces(table, gap):
    high = table.astype(jnp.bfloat16).astype(jnp.float32)
    rest = table - high
    middle = rest.astype(jnp.bfloat16).astype(jnp.float32)
    low = rest - middle
    return (high + pltpu.roll(middle, gap, 1) + pltpu.roll(low, 2 * gap, 1)).astype(jnp.bfloat16)


def load_kernel(bands, d_hbm, x_hbm, m_hbm, x_ref, m_ref, out_ref, days_ref, sems):
    dates, pixels = m_ref.shape
    mask_copy = pltpu.make_async_copy(m_hbm, m_ref, sems.at[0])
    mask_copy.start()
    value_copy = pltpu.make_async_copy(x_hbm, x_ref, sems.at[1])
    value_copy.start()
    days_copy = pltpu.make_async_copy(d_hbm, days_ref, sems.at[2])
    days_copy.start()
    shape = (dates, lanes)
    column = lax.broadcasted_iota(jnp.int32, shape, 1)
    row = lax.broadcasted_iota(jnp.int32, shape, 0)
    mask_copy.wait()
    value_copy.wait()
    step = 4 * lanes if pixels % (4 * lanes) == 0 else lanes
    totals = [jnp.zeros((dates, step), jnp.float32)] * (bands + 1)
    for at in range(0, pixels, step):
        valid = m_ref[:, at : at + step] > 0
        totals[bands] += jnp.where(valid, 1.0, 0.0)
        for b in range(bands):
            totals[b] += jnp.where(valid, x_ref[b, :, at : at + step].astype(jnp.float32), 0.0)
    table = jnp.zeros(shape, jnp.float32)
    days_copy.wait()
    for d in range(dates):
        table = jnp.where((row == d) & (column == bands + 1), days_ref[d].astype(jnp.float32), table)
    for b, total in enumerate(totals):
        table = jnp.where(column == b, jnp.sum(total, 1, keepdims=True), table)
    out_ref[...] = table


def pack_kernel(bands, groups, x_ref, m_ref, out_ref):
    dates, _ = m_ref.shape
    width = groups * lanes
    for c in range(out_ref.shape[0]):
        valid = m_ref[:, c * width : (c + 1) * width] > 0
        for b in range(bands):
            value = x_ref[b, :, c * width : (c + 1) * width].astype(jnp.float32)
            marked = jnp.where(valid, value, sentinel).astype(jnp.bfloat16)
            for g in range(groups):
                out_ref[c, b * groups + g] = marked[:, g * lanes : (g + 1) * lanes]


def stamp_kernel(bands, lines, own_ref, other_ref, in_ref, out_ref):
    del in_ref
    own = own_ref[...]
    total = own + other_ref[...]
    dates = total.shape[0]
    column = lax.broadcasted_iota(jnp.int32, total.shape, 1)
    count = jnp.sum(jnp.where(column == bands, total, 0.0), 1, keepdims=True)
    stats = jnp.where(column < bands, total / jnp.maximum(count, 1.0), 0.0)
    stats = split_pieces(jnp.where(column == bands + 1, own / 365.0, stats), bands + 2)
    for c in range(out_ref.shape[0]):
        out_ref[c, lines] = stats


def merge_pairs(n):
    pairs = []

    def merge(lo, length, step):
        jump = step * 2
        if jump < length:
            merge(lo, length, jump)
            merge(lo + step, length, jump)
            for i in range(lo + step, lo + length - step, jump):
                pairs.append((i, i + step))
        else:
            pairs.append((lo, lo + step))

    def sort(lo, length):
        if length > 1:
            half = length // 2
            sort(lo, half)
            sort(lo + half, half)
            merge(lo, length, 1)

    sort(0, n)
    return pairs


def sort_list(items):
    items = list(items)
    n = 1
    while n < len(items):
        n *= 2
    for i, j in merge_pairs(n):
        if j < len(items):
            items[i], items[j] = jnp.minimum(items[i], items[j]), jnp.maximum(items[i], items[j])
    return items


def middle_of(values, shape):
    half = len(values) // 2
    size = shape[0]
    pair = (2 * size, shape[1])
    upper = lax.broadcasted_iota(jnp.int32, pair, 0) < size
    sign = jnp.where(upper, big, -big).astype(jnp.bfloat16)
    items = []
    for first, second in zip(values[:half], values[half:]):
        value = jnp.concatenate([first, second], 0).astype(jnp.bfloat16)
        clear = value < limit
        items.append(jnp.where(clear, value, sign))
        sign = jnp.where(clear, sign, -sign)
    items = [item.astype(jnp.float32) for item in sort_list(items)]
    sign = sign.astype(jnp.float32)
    odd_first, odd_second = sign[:size] < 0, sign[size:] > 0
    low = functools.reduce(jnp.maximum, [jnp.minimum(items[i][:size], items[half - 1 - i][size:]) for i in range(half)])
    high = functools.reduce(jnp.minimum, [jnp.maximum(items[i][:size], items[half - 1 - i][size:]) for i in range(half)])
    left = jnp.where(odd_second & ~odd_first, high, low)
    right = jnp.where(odd_first & ~odd_second, low, high)
    return 0.5 * (left + right)


def blocks_of(lines):
    return [(start, min(8, lines - start)) for start in range(0, lines, 8)]


def fit_kernel(bands, groups, dates, in_ref, out_ref, wide_ref, table_ref):
    sources = in_ref.shape[0]
    lines = bands * groups
    rows = lines * dates
    gap = bands + 2
    wide = (lanes, (bands + 1) * lanes)
    pick = lax.broadcasted_iota(jnp.int32, wide, 0)
    to = lax.broadcasted_iota(jnp.int32, wide, 1) // lanes
    to = jnp.where(to == bands, bands + 1, to)
    spread = ((pick == to) | (pick == to + gap) | (pick == to + 2 * gap)).astype(jnp.bfloat16)
    for s in range(sources):
        for line in range(lines):
            wide_ref[s, line * dates : (line + 1) * dates, :] = in_ref[s, line].astype(jnp.float32)
    stats = jnp.concatenate([in_ref[s, lines] for s in range(sources)], 0)
    table_ref[...] = jnp.dot(stats, spread, preferred_element_type=jnp.float32)
    shared = None
    for start, size in blocks_of(lines):
        shape = (size, lanes)
        line = lax.broadcasted_iota(jnp.int32, shape, 0) + start
        fresh = shared is None or 8 % groups != 0 or shared[0].shape != shape
        zero = jnp.zeros(shape, jnp.float32)
        s_y, s_ty, s_zero, s_one, s_two = zero, zero, zero, zero, zero
        values = []
        for s in range(sources):
            for d in range(dates):

                def stat_at(b):
                    at = s * dates + d
                    row = table_ref[at : at + 1, b * lanes : (b + 1) * lanes]
                    return jnp.broadcast_to(row, shape)

                mean = stat_at(start // groups)
                for b in range(start // groups + 1, (start + size - 1) // groups + 1):
                    mean = jnp.where(line >= b * groups, stat_at(b), mean)
                value = wide_ref[s, pl.ds(start * dates + d, size, stride=dates), :]
                values.append(value)
                clear = value < limit
                year = stat_at(bands)
                part = jnp.where(clear, value - mean, 0.0)
                s_y = s_y + part
                s_ty = s_ty + year * part
                if fresh:
                    timed = jnp.where(clear, year, 0.0)
                    s_zero = s_zero + jnp.where(clear, 1.0, 0.0)
                    s_one = s_one + timed
                    s_two = s_two + timed * year
        median = middle_of(values, shape)
        if fresh:
            first = s_zero + ridge
            shared = (first, s_one, first * (s_two + ridge) - s_one * s_one)
        first, s_one, determinant = shared
        slope = (first * s_ty - s_one * s_y) / determinant
        for c in range(out_ref.shape[0]):
            out_ref[c, start : start + size, :] = median
            out_ref[c, lines + start : lines + start + size, :] = slope


def place_kernel(bands, groups, turns, in_ref, median_ref, slope_ref, held_ref, sems):
    lines = bands * groups
    copies = []
    for n, to_ref in enumerate((median_ref, slope_ref)):
        for s, part in enumerate(turns):
            for g in range(groups):
                at = (part * groups + g) * lanes
                held_ref[n, :, at : at + lanes] = in_ref[s, pl.ds(n * lines + g, bands, stride=groups), :]
        copy = pltpu.make_async_copy(held_ref.at[n], to_ref, sems.at[n])
        copy.start()
        copies.append(copy)
    for copy in copies:
        copy.wait()


def call(kernel, name, out_shape, in_specs, scratch=(), flops=0, aliases={}, space=pltpu.VMEM):
    many = isinstance(out_shape, tuple)
    spec = pl.BlockSpec(memory_space=space)
    cost = pl.CostEstimate(flops=flops, bytes_accessed=flops, transcendentals=0) if flops else None
    return pl.pallas_call(
        kernel,
        out_shape=out_shape,
        in_specs=[pl.BlockSpec(memory_space=space) for space in in_specs],
        out_specs=tuple([spec] * len(out_shape)) if many else spec,
        scratch_shapes=scratch,
        compiler_params=pltpu.CompilerParams(vmem_limit_bytes=8 * 1024 * 1024),
        cost_estimate=cost,
        input_output_aliases=aliases,
        name=name,
    )


def tuned(parts, tiles):
    return len(orders) == tiles and len(again) == parts


def exchange(x, turn, tiles):
    if not tuned(x.shape[0], tiles):
        return lax.all_to_all(x, "date", split_axis=0, concat_axis=0, tiled=True)
    groups = [[order[i] * tiles + tile for i in turn] for tile, order in enumerate(orders)]
    return lax.all_to_all(x, ("date", "pix"), split_axis=0, concat_axis=0, tiled=True, axis_index_groups=groups)


def local(parts, tiles, reflect, cloud_free, days):
    dates, bands, pixels = reflect.shape
    groups = pixels // parts // lanes
    lines = bands * groups
    rows = lines * dates
    inside, outside = pltpu.VMEM, pltpu.HBM
    array = jax.ShapeDtypeStruct
    values = jnp.transpose(reflect, (1, 0, 2))
    held, mask, own = call(
        functools.partial(load_kernel, bands),
        "load",
        (
            array(values.shape, values.dtype),
            array(cloud_free.shape, cloud_free.dtype),
            array((dates, lanes), jnp.float32),
        ),
        [outside if dates > 1 else pl.ANY, outside, outside],
        [pltpu.SMEM((dates,), jnp.int32), pltpu.SemaphoreType.DMA((3,))],
    )(*[pltpu.with_memory_space_constraint(x, outside) if x.size > 1 else x for x in (days, values, cloud_free)])
    if tiles == 2:
        other = lax.ppermute(own, "pix", [(0, 1), (1, 0)])
    else:
        ring = [(i, (i + 1) % tiles) for i in range(tiles)]
        passed, other = own, jnp.zeros(own.shape, own.dtype)
        for _ in range(tiles - 1):
            passed = lax.ppermute(passed, "pix", ring)
            other = other + passed
    packed = call(
        functools.partial(pack_kernel, bands, groups),
        "pack",
        array((parts, lines + 1, dates, lanes), jnp.bfloat16),
        [inside, inside],
        flops=16_000_000,
    )(held, mask)
    stamped = call(
        functools.partial(stamp_kernel, bands, lines),
        "stamp",
        array(packed.shape, packed.dtype),
        [inside] * 3,
        aliases={2: 0},
    )(own, other, pltpu.with_memory_space_constraint(packed, inside))
    turns = again if tuned(parts, tiles) else tuple(range(parts))
    moved = exchange(stamped, tuple(range(parts)), tiles)
    fitted = call(
        functools.partial(fit_kernel, bands, groups, dates),
        "fit",
        array((parts, 2 * lines, lanes), jnp.float32),
        [inside],
        [
            pltpu.VMEM((parts, rows, lanes), jnp.float32),
            pltpu.VMEM((parts * dates, (bands + 1) * lanes), jnp.float32),
        ],
    )(moved)
    spread = exchange(fitted, turns, tiles)
    shape = array((bands, pixels), jnp.float32)
    return call(
        functools.partial(place_kernel, bands, groups, turns),
        "place",
        (shape, shape),
        [inside],
        [pltpu.VMEM((2, bands, pixels), jnp.float32), pltpu.SemaphoreType.DMA((2,))],
        space=outside,
    )(spread)


def solution(mesh):
    placed = (P("date", None, "pix"), P("date", "pix"), P("date"))
    return jax.shard_map(
        functools.partial(local, mesh.shape["date"], mesh.shape["pix"]),
        mesh=mesh,
        in_specs=placed,
        out_specs=(P(None, "pix"), P(None, "pix")),
        check_vma=False,
    )
```

```python
import functools

import jax
import jax.numpy as jnp
from jax import lax
from jax.experimental import pallas as pl
from jax.experimental.pallas import tpu as pltpu
from jax.sharding import PartitionSpec as P

ridge = 1.0
sentinel = 100.0
limit = 50.0
big = 1000.0
lanes = 128
orders = (
    (0, 12, 5, 8, 14, 11, 10, 2, 15, 6, 9, 1, 3, 7, 4, 13),
    (11, 0, 15, 1, 13, 8, 3, 6, 7, 2, 10, 4, 14, 5, 12, 9),
)
again = (5, 8, 7, 9, 0, 12, 10, 11, 2, 13, 6, 4, 1, 14, 15, 3)


def split_pieces(table, gap):
    high = table.astype(jnp.bfloat16).astype(jnp.float32)
    rest = table - high
    middle = rest.astype(jnp.bfloat16).astype(jnp.float32)
    low = rest - middle
    return (high + pltpu.roll(middle, gap, 1) + pltpu.roll(low, 2 * gap, 1)).astype(jnp.bfloat16)


def load_kernel(bands, d_hbm, x_hbm, m_hbm, x_ref, m_ref, out_ref, days_ref, sems):
    dates, pixels = m_ref.shape
    mask_copy = pltpu.make_async_copy(m_hbm, m_ref, sems.at[0])
    mask_copy.start()
    value_copy = pltpu.make_async_copy(x_hbm, x_ref, sems.at[1])
    value_copy.start()
    days_copy = pltpu.make_async_copy(d_hbm, days_ref, sems.at[2])
    days_copy.start()
    shape = (dates, lanes)
    column = lax.broadcasted_iota(jnp.int32, shape, 1)
    row = lax.broadcasted_iota(jnp.int32, shape, 0)
    mask_copy.wait()
    value_copy.wait()
    step = 4 * lanes if pixels % (4 * lanes) == 0 else lanes
    totals = [jnp.zeros((dates, step), jnp.float32)] * (bands + 1)
    for at in range(0, pixels, step):
        valid = m_ref[:, at : at + step] > 0
        totals[bands] += jnp.where(valid, 1.0, 0.0)
        for b in range(bands):
            totals[b] += jnp.where(valid, x_ref[b, :, at : at + step].astype(jnp.float32), 0.0)
    table = jnp.zeros(shape, jnp.float32)
    days_copy.wait()
    for d in range(dates):
        table = jnp.where((row == d) & (column == bands + 1), days_ref[d].astype(jnp.float32), table)
    for b, total in enumerate(totals):
        table = jnp.where(column == b, jnp.sum(total, 1, keepdims=True), table)
    out_ref[...] = table


def pack_kernel(bands, groups, x_ref, m_ref, out_ref):
    dates, _ = m_ref.shape
    width = groups * lanes
    for c in range(out_ref.shape[0]):
        valid = m_ref[:, c * width : (c + 1) * width] > 0
        for b in range(bands):
            value = x_ref[b, :, c * width : (c + 1) * width].astype(jnp.float32)
            marked = jnp.where(valid, value, sentinel).astype(jnp.bfloat16)
            for g in range(groups):
                out_ref[c, b * groups + g] = marked[:, g * lanes : (g + 1) * lanes]


def stamp_kernel(bands, lines, own_ref, other_ref, in_ref, out_ref):
    del in_ref
    own = own_ref[...]
    total = own + other_ref[...]
    dates = total.shape[0]
    column = lax.broadcasted_iota(jnp.int32, total.shape, 1)
    count = jnp.sum(jnp.where(column == bands, total, 0.0), 1, keepdims=True)
    stats = jnp.where(column < bands, total / jnp.maximum(count, 1.0), 0.0)
    stats = split_pieces(jnp.where(column == bands + 1, own / 365.0, stats), bands + 2)
    for c in range(out_ref.shape[0]):
        out_ref[c, lines] = stats


def merge_pairs(n):
    pairs = []

    def merge(lo, length, step):
        jump = step * 2
        if jump < length:
            merge(lo, length, jump)
            merge(lo + step, length, jump)
            for i in range(lo + step, lo + length - step, jump):
                pairs.append((i, i + step))
        else:
            pairs.append((lo, lo + step))

    def sort(lo, length):
        if length > 1:
            half = length // 2
            sort(lo, half)
            sort(lo + half, half)
            merge(lo, length, 1)

    sort(0, n)
    return pairs


def sort_list(items):
    items = list(items)
    n = 1
    while n < len(items):
        n *= 2
    for i, j in merge_pairs(n):
        if j < len(items):
            items[i], items[j] = jnp.minimum(items[i], items[j]), jnp.maximum(items[i], items[j])
    return items


def middle_of(values, shape):
    half = len(values) // 2
    size = shape[0]
    pair = (2 * size, shape[1])
    upper = lax.broadcasted_iota(jnp.int32, pair, 0) < size
    sign = jnp.where(upper, big, -big).astype(jnp.bfloat16)
    items = []
    for first, second in zip(values[:half], values[half:]):
        value = jnp.concatenate([first, second], 0).astype(jnp.bfloat16)
        clear = value < limit
        items.append(jnp.where(clear, value, sign))
        sign = jnp.where(clear, sign, -sign)
    items = [item.astype(jnp.float32) for item in sort_list(items)]
    sign = sign.astype(jnp.float32)
    odd_first, odd_second = sign[:size] < 0, sign[size:] > 0
    low = functools.reduce(jnp.maximum, [jnp.minimum(items[i][:size], items[half - 1 - i][size:]) for i in range(half)])
    high = functools.reduce(jnp.minimum, [jnp.maximum(items[i][:size], items[half - 1 - i][size:]) for i in range(half)])
    left = jnp.where(odd_second & ~odd_first, high, low)
    right = jnp.where(odd_first & ~odd_second, low, high)
    return 0.5 * (left + right)


def blocks_of(lines):
    return [(start, min(8, lines - start)) for start in range(0, lines, 8)]


def fit_kernel(bands, groups, dates, in_ref, out_ref, wide_ref, table_ref):
    sources = in_ref.shape[0]
    lines = bands * groups
    rows = lines * dates
    gap = bands + 2
    wide = (lanes, (bands + 1) * lanes)
    pick = lax.broadcasted_iota(jnp.int32, wide, 0)
    to = lax.broadcasted_iota(jnp.int32, wide, 1) // lanes
    to = jnp.where(to == bands, bands + 1, to)
    spread = ((pick == to) | (pick == to + gap) | (pick == to + 2 * gap)).astype(jnp.bfloat16)
    for s in range(sources):
        wide_ref[s] = in_ref[s, 0:lines].astype(jnp.float32).reshape(rows, lanes)
    stats = jnp.concatenate([in_ref[s, lines] for s in range(sources)], 0)
    table_ref[...] = jnp.dot(stats, spread, preferred_element_type=jnp.float32)
    shared = None
    for start, size in blocks_of(lines):
        shape = (size, lanes)
        line = lax.broadcasted_iota(jnp.int32, shape, 0) + start
        fresh = shared is None or 8 % groups != 0 or shared[0].shape != shape
        zero = jnp.zeros(shape, jnp.float32)
        s_y, s_ty, s_zero, s_one, s_two = zero, zero, zero, zero, zero
        values = []
        for s in range(sources):
            for d in range(dates):

                def stat_at(b):
                    at = s * dates + d
                    row = table_ref[at : at + 1, b * lanes : (b + 1) * lanes]
                    return jnp.broadcast_to(row, shape)

                mean = stat_at(start // groups)
                for b in range(start // groups + 1, (start + size - 1) // groups + 1):
                    mean = jnp.where(line >= b * groups, stat_at(b), mean)
                value = wide_ref[s, pl.ds(start * dates + d, size, stride=dates), :]
                values.append(value)
                clear = value < limit
                year = stat_at(bands)
                part = jnp.where(clear, value - mean, 0.0)
                s_y = s_y + part
                s_ty = s_ty + year * part
                if fresh:
                    timed = jnp.where(clear, year, 0.0)
                    s_zero = s_zero + jnp.where(clear, 1.0, 0.0)
                    s_one = s_one + timed
                    s_two = s_two + timed * year
        median = middle_of(values, shape)
        if fresh:
            first = s_zero + ridge
            shared = (first, s_one, first * (s_two + ridge) - s_one * s_one)
        first, s_one, determinant = shared
        slope = (first * s_ty - s_one * s_y) / determinant
        for c in range(out_ref.shape[0]):
            out_ref[c, start : start + size, :] = median
            out_ref[c, lines + start : lines + start + size, :] = slope


def place_kernel(bands, groups, turns, in_ref, median_ref, slope_ref, held_ref, sems):
    lines = bands * groups
    copies = []
    for n, to_ref in enumerate((median_ref, slope_ref)):
        for s, part in enumerate(turns):
            for g in range(groups):
                at = (part * groups + g) * lanes
                held_ref[n, :, at : at + lanes] = in_ref[s, pl.ds(n * lines + g, bands, stride=groups), :]
        copy = pltpu.make_async_copy(held_ref.at[n], to_ref, sems.at[n])
        copy.start()
        copies.append(copy)
    for copy in copies:
        copy.wait()


def call(kernel, name, out_shape, in_specs, scratch=(), flops=0, aliases={}, space=pltpu.VMEM):
    many = isinstance(out_shape, tuple)
    spec = pl.BlockSpec(memory_space=space)
    cost = pl.CostEstimate(flops=flops, bytes_accessed=flops, transcendentals=0) if flops else None
    return pl.pallas_call(
        kernel,
        out_shape=out_shape,
        in_specs=[pl.BlockSpec(memory_space=space) for space in in_specs],
        out_specs=tuple([spec] * len(out_shape)) if many else spec,
        scratch_shapes=scratch,
        compiler_params=pltpu.CompilerParams(vmem_limit_bytes=8 * 1024 * 1024),
        cost_estimate=cost,
        input_output_aliases=aliases,
        name=name,
    )


def tuned(parts, tiles):
    return len(orders) == tiles and len(again) == parts


def exchange(x, turn, tiles):
    if not tuned(x.shape[0], tiles):
        return lax.all_to_all(x, "date", split_axis=0, concat_axis=0, tiled=True)
    groups = [[order[i] * tiles + tile for i in turn] for tile, order in enumerate(orders)]
    return lax.all_to_all(x, ("date", "pix"), split_axis=0, concat_axis=0, tiled=True, axis_index_groups=groups)


def local(parts, tiles, reflect, cloud_free, days):
    dates, bands, pixels = reflect.shape
    groups = pixels // parts // lanes
    lines = bands * groups
    rows = lines * dates
    inside, outside = pltpu.VMEM, pltpu.HBM
    array = jax.ShapeDtypeStruct
    values = jnp.transpose(reflect, (1, 0, 2))
    held, mask, own = call(
        functools.partial(load_kernel, bands),
        "load",
        (
            array(values.shape, values.dtype),
            array(cloud_free.shape, cloud_free.dtype),
            array((dates, lanes), jnp.float32),
        ),
        [outside if dates > 1 else pl.ANY, outside, outside],
        [pltpu.SMEM((dates,), jnp.int32), pltpu.SemaphoreType.DMA((3,))],
    )(*[pltpu.with_memory_space_constraint(x, outside) if x.size > 1 else x for x in (days, values, cloud_free)])
    if tiles == 2:
        other = lax.ppermute(own, "pix", [(0, 1), (1, 0)])
    else:
        ring = [(i, (i + 1) % tiles) for i in range(tiles)]
        passed, other = own, jnp.zeros(own.shape, own.dtype)
        for _ in range(tiles - 1):
            passed = lax.ppermute(passed, "pix", ring)
            other = other + passed
    packed = call(
        functools.partial(pack_kernel, bands, groups),
        "pack",
        array((parts, lines + 1, dates, lanes), jnp.bfloat16),
        [inside, inside],
        flops=16_000_000,
    )(held, mask)
    stamped = call(
        functools.partial(stamp_kernel, bands, lines),
        "stamp",
        array(packed.shape, packed.dtype),
        [inside] * 3,
        aliases={2: 0},
    )(own, other, pltpu.with_memory_space_constraint(packed, inside))
    turns = again if tuned(parts, tiles) else tuple(range(parts))
    moved = exchange(stamped, tuple(range(parts)), tiles)
    fitted = call(
        functools.partial(fit_kernel, bands, groups, dates),
        "fit",
        array((parts, 2 * lines, lanes), jnp.float32),
        [inside],
        [
            pltpu.VMEM((parts, rows, lanes), jnp.float32),
            pltpu.VMEM((parts * dates, (bands + 1) * lanes), jnp.float32),
        ],
    )(moved)
    spread = exchange(fitted, turns, tiles)
    shape = array((bands, pixels), jnp.float32)
    return call(
        functools.partial(place_kernel, bands, groups, turns),
        "place",
        (shape, shape),
        [inside],
        [pltpu.VMEM((2, bands, pixels), jnp.float32), pltpu.SemaphoreType.DMA((2,))],
        space=outside,
    )(spread)


def solution(mesh):
    placed = (P("date", None, "pix"), P("date", "pix"), P("date"))
    return jax.shard_map(
        functools.partial(local, mesh.shape["date"], mesh.shape["pix"]),
        mesh=mesh,
        in_specs=placed,
        out_specs=(P(None, "pix"), P(None, "pix")),
        check_vma=False,
    )
```

```python
import functools

import jax
import jax.numpy as jnp
from jax import lax
from jax.experimental import pallas as pl
from jax.experimental.pallas import tpu as pltpu
from jax.sharding import PartitionSpec as P

ridge = 1.0
sentinel = 100.0
limit = 50.0
big = 1000.0
lanes = 128
orders = (
    (0, 12, 5, 8, 14, 11, 10, 2, 15, 6, 9, 1, 3, 7, 4, 13),
    (11, 0, 15, 1, 13, 8, 3, 6, 7, 2, 10, 4, 14, 5, 12, 9),
)
again = (5, 8, 7, 9, 0, 12, 10, 11, 2, 13, 6, 4, 1, 14, 15, 3)


def split_pieces(table, gap):
    high = table.astype(jnp.bfloat16).astype(jnp.float32)
    rest = table - high
    middle = rest.astype(jnp.bfloat16).astype(jnp.float32)
    low = rest - middle
    return (high + pltpu.roll(middle, gap, 1) + pltpu.roll(low, 2 * gap, 1)).astype(jnp.bfloat16)


def load_kernel(bands, d_hbm, x_hbm, m_hbm, x_ref, m_ref, out_ref, days_ref, sems):
    dates, pixels = m_ref.shape
    mask_copy = pltpu.make_async_copy(m_hbm, m_ref, sems.at[0])
    mask_copy.start()
    value_copy = pltpu.make_async_copy(x_hbm, x_ref, sems.at[1])
    value_copy.start()
    days_copy = pltpu.make_async_copy(d_hbm, days_ref, sems.at[2])
    days_copy.start()
    shape = (dates, lanes)
    column = lax.broadcasted_iota(jnp.int32, shape, 1)
    row = lax.broadcasted_iota(jnp.int32, shape, 0)
    mask_copy.wait()
    value_copy.wait()
    step = 4 * lanes if pixels % (4 * lanes) == 0 else lanes
    totals = [jnp.zeros((dates, step), jnp.float32)] * (bands + 1)
    for at in range(0, pixels, step):
        valid = m_ref[:, at : at + step] > 0
        totals[bands] += jnp.where(valid, 1.0, 0.0)
        for b in range(bands):
            totals[b] += jnp.where(valid, x_ref[b, :, at : at + step].astype(jnp.float32), 0.0)
    table = jnp.zeros(shape, jnp.float32)
    days_copy.wait()
    for d in range(dates):
        table = jnp.where((row == d) & (column == bands + 1), days_ref[d].astype(jnp.float32), table)
    for b, total in enumerate(totals):
        table = jnp.where(column == b, jnp.sum(total, 1, keepdims=True), table)
    out_ref[...] = table


def pack_kernel(bands, groups, x_ref, m_ref, out_ref):
    dates, _ = m_ref.shape
    width = groups * lanes
    for c in range(out_ref.shape[0]):
        valid = m_ref[:, c * width : (c + 1) * width] > 0
        for b in range(bands):
            value = x_ref[b, :, c * width : (c + 1) * width].astype(jnp.float32)
            marked = jnp.where(valid, value, sentinel).astype(jnp.bfloat16)
            for g in range(groups):
                out_ref[c, b * groups + g] = marked[:, g * lanes : (g + 1) * lanes]


def stamp_kernel(bands, lines, own_ref, other_ref, in_ref, out_ref):
    del in_ref
    own = own_ref[...]
    total = own + other_ref[...]
    dates = total.shape[0]
    column = lax.broadcasted_iota(jnp.int32, total.shape, 1)
    count = jnp.sum(jnp.where(column == bands, total, 0.0), 1, keepdims=True)
    stats = jnp.where(column < bands, total / jnp.maximum(count, 1.0), 0.0)
    stats = split_pieces(jnp.where(column == bands + 1, own / 365.0, stats), bands + 2)
    for c in range(out_ref.shape[0]):
        out_ref[c, lines] = stats


def merge_pairs(n):
    pairs = []

    def merge(lo, length, step):
        jump = step * 2
        if jump < length:
            merge(lo, length, jump)
            merge(lo + step, length, jump)
            for i in range(lo + step, lo + length - step, jump):
                pairs.append((i, i + step))
        else:
            pairs.append((lo, lo + step))

    def sort(lo, length):
        if length > 1:
            half = length // 2
            sort(lo, half)
            sort(lo + half, half)
            merge(lo, length, 1)

    sort(0, n)
    return pairs


def sort_list(items):
    items = list(items)
    n = 1
    while n < len(items):
        n *= 2
    for i, j in merge_pairs(n):
        if j < len(items):
            items[i], items[j] = jnp.minimum(items[i], items[j]), jnp.maximum(items[i], items[j])
    return items


def middle_of(values, shape):
    half = len(values) // 2
    size = shape[0]
    pair = (2 * size, shape[1])
    upper = lax.broadcasted_iota(jnp.int32, pair, 0) < size
    sign = jnp.where(upper, big, -big).astype(jnp.bfloat16)
    items = []
    for first, second in zip(values[:half], values[half:]):
        value = jnp.concatenate([first, second], 0).astype(jnp.bfloat16)
        clear = value < limit
        items.append(jnp.where(clear, value, sign))
        sign = jnp.where(clear, sign, -sign)
    items = sort_list(items)
    sign = sign.astype(jnp.float32)
    odd_first, odd_second = sign[:size] < 0, sign[size:] > 0
    near = items[: (half + 1) // 2]
    far = [jnp.concatenate([item[size:], item[:size]], 0) for item in items[half // 2 :][::-1]]
    low = functools.reduce(jnp.maximum, [jnp.minimum(x, y) for x, y in zip(near, far)]).astype(jnp.float32)
    high = functools.reduce(jnp.minimum, [jnp.maximum(x, y) for x, y in zip(near, far)]).astype(jnp.float32)
    low = jnp.maximum(low[:size], low[size:])
    high = jnp.minimum(high[:size], high[size:])
    left = jnp.where(odd_second & ~odd_first, high, low)
    right = jnp.where(odd_first & ~odd_second, low, high)
    return 0.5 * (left + right)


def blocks_of(lines):
    return [(start, min(8, lines - start)) for start in range(0, lines, 8)]


def fit_kernel(bands, groups, dates, in_ref, out_ref, wide_ref, table_ref):
    sources = in_ref.shape[0]
    lines = bands * groups
    rows = lines * dates
    gap = bands + 2
    wide = (lanes, (bands + 1) * lanes)
    pick = lax.broadcasted_iota(jnp.int32, wide, 0)
    to = lax.broadcasted_iota(jnp.int32, wide, 1) // lanes
    to = jnp.where(to == bands, bands + 1, to)
    spread = ((pick == to) | (pick == to + gap) | (pick == to + 2 * gap)).astype(jnp.bfloat16)
    for s in range(sources):
        wide_ref[s] = in_ref[s, 0:lines].astype(jnp.float32).reshape(rows, lanes)
    stats = jnp.concatenate([in_ref[s, lines] for s in range(sources)], 0)
    table_ref[...] = jnp.dot(stats, spread, preferred_element_type=jnp.float32)
    shared = None
    for start, size in blocks_of(lines):
        shape = (size, lanes)
        line = lax.broadcasted_iota(jnp.int32, shape, 0) + start
        fresh = shared is None or 8 % groups != 0 or shared[0].shape != shape
        zero = jnp.zeros(shape, jnp.float32)
        s_y, s_ty, s_zero, s_one, s_two = zero, zero, zero, zero, zero
        values = []
        for s in range(sources):
            for d in range(dates):

                def stat_at(b):
                    at = s * dates + d
                    row = table_ref[at : at + 1, b * lanes : (b + 1) * lanes]
                    return jnp.broadcast_to(row, shape)

                mean = stat_at(start // groups)
                for b in range(start // groups + 1, (start + size - 1) // groups + 1):
                    mean = jnp.where(line >= b * groups, stat_at(b), mean)
                value = wide_ref[s, pl.ds(start * dates + d, size, stride=dates), :]
                values.append(value)
                clear = value < limit
                year = stat_at(bands)
                part = jnp.where(clear, value - mean, 0.0)
                s_y = s_y + part
                s_ty = s_ty + year * part
                if fresh:
                    timed = jnp.where(clear, year, 0.0)
                    s_zero = s_zero + jnp.where(clear, 1.0, 0.0)
                    s_one = s_one + timed
                    s_two = s_two + timed * year
        median = middle_of(values, shape)
        if fresh:
            first = s_zero + ridge
            shared = (first, s_one, first * (s_two + ridge) - s_one * s_one)
        first, s_one, determinant = shared
        slope = (first * s_ty - s_one * s_y) / determinant
        for c in range(out_ref.shape[0]):
            out_ref[c, start : start + size, :] = median
            out_ref[c, lines + start : lines + start + size, :] = slope


def place_kernel(bands, groups, turns, in_ref, median_ref, slope_ref, held_ref, sems):
    lines = bands * groups
    copies = []
    for n, to_ref in enumerate((median_ref, slope_ref)):
        for s, part in enumerate(turns):
            for g in range(groups):
                at = (part * groups + g) * lanes
                held_ref[n, :, at : at + lanes] = in_ref[s, pl.ds(n * lines + g, bands, stride=groups), :]
        copy = pltpu.make_async_copy(held_ref.at[n], to_ref, sems.at[n])
        copy.start()
        copies.append(copy)
    for copy in copies:
        copy.wait()


def call(kernel, name, out_shape, in_specs, scratch=(), flops=0, aliases={}, space=pltpu.VMEM):
    many = isinstance(out_shape, tuple)
    spec = pl.BlockSpec(memory_space=space)
    cost = pl.CostEstimate(flops=flops, bytes_accessed=flops, transcendentals=0) if flops else None
    return pl.pallas_call(
        kernel,
        out_shape=out_shape,
        in_specs=[pl.BlockSpec(memory_space=space) for space in in_specs],
        out_specs=tuple([spec] * len(out_shape)) if many else spec,
        scratch_shapes=scratch,
        compiler_params=pltpu.CompilerParams(vmem_limit_bytes=8 * 1024 * 1024),
        cost_estimate=cost,
        input_output_aliases=aliases,
        name=name,
    )


def tuned(parts, tiles):
    return len(orders) == tiles and len(again) == parts


def exchange(x, turn, tiles):
    if not tuned(x.shape[0], tiles):
        return lax.all_to_all(x, "date", split_axis=0, concat_axis=0, tiled=True)
    groups = [[order[i] * tiles + tile for i in turn] for tile, order in enumerate(orders)]
    return lax.all_to_all(x, ("date", "pix"), split_axis=0, concat_axis=0, tiled=True, axis_index_groups=groups)


def local(parts, tiles, reflect, cloud_free, days):
    dates, bands, pixels = reflect.shape
    groups = pixels // parts // lanes
    lines = bands * groups
    rows = lines * dates
    inside, outside = pltpu.VMEM, pltpu.HBM
    array = jax.ShapeDtypeStruct
    values = jnp.transpose(reflect, (1, 0, 2))
    held, mask, own = call(
        functools.partial(load_kernel, bands),
        "load",
        (
            array(values.shape, values.dtype),
            array(cloud_free.shape, cloud_free.dtype),
            array((dates, lanes), jnp.float32),
        ),
        [outside if dates > 1 else pl.ANY, outside, outside],
        [pltpu.SMEM((dates,), jnp.int32), pltpu.SemaphoreType.DMA((3,))],
    )(*[pltpu.with_memory_space_constraint(x, outside) if x.size > 1 else x for x in (days, values, cloud_free)])
    if tiles == 2:
        other = lax.ppermute(own, "pix", [(0, 1), (1, 0)])
    else:
        ring = [(i, (i + 1) % tiles) for i in range(tiles)]
        passed, other = own, jnp.zeros(own.shape, own.dtype)
        for _ in range(tiles - 1):
            passed = lax.ppermute(passed, "pix", ring)
            other = other + passed
    packed = call(
        functools.partial(pack_kernel, bands, groups),
        "pack",
        array((parts, lines + 1, dates, lanes), jnp.bfloat16),
        [inside, inside],
        flops=16_000_000,
    )(held, mask)
    stamped = call(
        functools.partial(stamp_kernel, bands, lines),
        "stamp",
        array(packed.shape, packed.dtype),
        [inside] * 3,
        aliases={2: 0},
    )(own, other, pltpu.with_memory_space_constraint(packed, inside))
    turns = again if tuned(parts, tiles) else tuple(range(parts))
    moved = exchange(stamped, tuple(range(parts)), tiles)
    fitted = call(
        functools.partial(fit_kernel, bands, groups, dates),
        "fit",
        array((parts, 2 * lines, lanes), jnp.float32),
        [inside],
        [
            pltpu.VMEM((parts, rows, lanes), jnp.float32),
            pltpu.VMEM((parts * dates, (bands + 1) * lanes), jnp.float32),
        ],
    )(moved)
    spread = exchange(fitted, turns, tiles)
    shape = array((bands, pixels), jnp.float32)
    return call(
        functools.partial(place_kernel, bands, groups, turns),
        "place",
        (shape, shape),
        [inside],
        [pltpu.VMEM((2, bands, pixels), jnp.float32), pltpu.SemaphoreType.DMA((2,))],
        space=outside,
    )(spread)


def solution(mesh):
    placed = (P("date", None, "pix"), P("date", "pix"), P("date"))
    return jax.shard_map(
        functools.partial(local, mesh.shape["date"], mesh.shape["pix"]),
        mesh=mesh,
        in_specs=placed,
        out_specs=(P(None, "pix"), P(None, "pix")),
        check_vma=False,
    )
```

```python
import functools

import jax
import jax.numpy as jnp
from jax import lax
from jax.experimental import pallas as pl
from jax.experimental.pallas import tpu as pltpu
from jax.sharding import PartitionSpec as P

ridge = 1.0
sentinel = 100.0
limit = 50.0
big = 1000.0
lanes = 128
orders = (
    (0, 12, 5, 8, 14, 11, 10, 2, 15, 6, 9, 1, 3, 7, 4, 13),
    (11, 0, 15, 1, 13, 8, 3, 6, 7, 2, 10, 4, 14, 5, 12, 9),
)
again = (5, 8, 7, 9, 0, 12, 10, 11, 2, 13, 6, 4, 1, 14, 15, 3)


def split_pieces(table, gap):
    high = table.astype(jnp.bfloat16).astype(jnp.float32)
    rest = table - high
    middle = rest.astype(jnp.bfloat16).astype(jnp.float32)
    low = rest - middle
    return (high + pltpu.roll(middle, gap, 1) + pltpu.roll(low, 2 * gap, 1)).astype(jnp.bfloat16)


def load_kernel(bands, d_hbm, x_hbm, m_hbm, x_ref, m_ref, out_ref, days_ref, sems):
    dates, pixels = m_ref.shape
    mask_copy = pltpu.make_async_copy(m_hbm, m_ref, sems.at[0])
    mask_copy.start()
    value_copy = pltpu.make_async_copy(x_hbm, x_ref, sems.at[1])
    value_copy.start()
    days_copy = pltpu.make_async_copy(d_hbm, days_ref, sems.at[2])
    days_copy.start()
    shape = (dates, lanes)
    column = lax.broadcasted_iota(jnp.int32, shape, 1)
    row = lax.broadcasted_iota(jnp.int32, shape, 0)
    mask_copy.wait()
    value_copy.wait()
    step = 4 * lanes if pixels % (4 * lanes) == 0 else lanes
    totals = [jnp.zeros((dates, step), jnp.float32)] * (bands + 1)
    for at in range(0, pixels, step):
        valid = m_ref[:, at : at + step] > 0
        totals[bands] += jnp.where(valid, 1.0, 0.0)
        for b in range(bands):
            totals[b] += jnp.where(valid, x_ref[b, :, at : at + step].astype(jnp.float32), 0.0)
    table = jnp.zeros(shape, jnp.float32)
    days_copy.wait()
    for d in range(dates):
        table = jnp.where((row == d) & (column == bands + 1), days_ref[d].astype(jnp.float32), table)
    for b, total in enumerate(totals):
        table = jnp.where(column == b, jnp.sum(total, 1, keepdims=True), table)
    out_ref[...] = table


def pack_kernel(bands, groups, x_ref, m_ref, out_ref):
    dates, _ = m_ref.shape
    width = groups * lanes
    for c in range(out_ref.shape[0]):
        valid = m_ref[:, c * width : (c + 1) * width] > 0
        for b in range(bands):
            value = x_ref[b, :, c * width : (c + 1) * width].astype(jnp.float32)
            marked = jnp.where(valid, value, sentinel).astype(jnp.bfloat16)
            for g in range(groups):
                out_ref[c, b * groups + g] = marked[:, g * lanes : (g + 1) * lanes]


def stamp_kernel(bands, lines, own_ref, other_ref, in_ref, out_ref):
    del in_ref
    own = own_ref[...]
    total = own + other_ref[...]
    dates = total.shape[0]
    column = lax.broadcasted_iota(jnp.int32, total.shape, 1)
    count = jnp.sum(jnp.where(column == bands, total, 0.0), 1, keepdims=True)
    stats = jnp.where(column < bands, total / jnp.maximum(count, 1.0), 0.0)
    stats = split_pieces(jnp.where(column == bands + 1, own / 365.0, stats), bands + 2)
    for c in range(out_ref.shape[0]):
        out_ref[c, lines] = stats


def merge_pairs(n):
    pairs = []

    def merge(lo, length, step):
        jump = step * 2
        if jump < length:
            merge(lo, length, jump)
            merge(lo + step, length, jump)
            for i in range(lo + step, lo + length - step, jump):
                pairs.append((i, i + step))
        else:
            pairs.append((lo, lo + step))

    def sort(lo, length):
        if length > 1:
            half = length // 2
            sort(lo, half)
            sort(lo + half, half)
            merge(lo, length, 1)

    sort(0, n)
    return pairs


def sort_list(items):
    items = list(items)
    n = 1
    while n < len(items):
        n *= 2
    for i, j in merge_pairs(n):
        if j < len(items):
            items[i], items[j] = jnp.minimum(items[i], items[j]), jnp.maximum(items[i], items[j])
    return items


def middle_of(values, shape):
    half = len(values) // 2
    size = shape[0]
    pair = (2 * size, shape[1])
    upper = lax.broadcasted_iota(jnp.int32, pair, 0) < size
    sign = jnp.where(upper, big, -big).astype(jnp.bfloat16)
    items = []
    for first, second in zip(values[:half], values[half:]):
        value = jnp.concatenate([first, second], 0).astype(jnp.bfloat16)
        clear = value < limit
        items.append(jnp.where(clear, value, sign))
        sign = jnp.where(clear, sign, -sign)
    items = sort_list(items)
    sign = sign.astype(jnp.float32)
    odd_first, odd_second = sign[:size] < 0, sign[size:] > 0
    near = items[: (half + 1) // 2]
    far = [jnp.concatenate([item[size:], item[:size]], 0) for item in items[half // 2 :][::-1]]
    low = functools.reduce(jnp.maximum, [jnp.minimum(x, y) for x, y in zip(near, far)]).astype(jnp.float32)
    high = functools.reduce(jnp.minimum, [jnp.maximum(x, y) for x, y in zip(near, far)]).astype(jnp.float32)
    low = jnp.maximum(low[:size], low[size:])
    high = jnp.minimum(high[:size], high[size:])
    left = jnp.where(odd_second & ~odd_first, high, low)
    right = jnp.where(odd_first & ~odd_second, low, high)
    return 0.5 * (left + right)


def blocks_of(lines):
    return [(start, min(8, lines - start)) for start in range(0, lines, 8)]


def fit_kernel(bands, groups, dates, in_ref, out_ref, wide_ref, table_ref):
    sources = in_ref.shape[0]
    lines = bands * groups
    rows = lines * dates
    gap = bands + 2
    wide = (lanes, (bands + 1) * lanes)
    pick = lax.broadcasted_iota(jnp.int32, wide, 0)
    to = lax.broadcasted_iota(jnp.int32, wide, 1) // lanes
    to = jnp.where(to == bands, bands + 1, to)
    spread = ((pick == to) | (pick == to + gap) | (pick == to + 2 * gap)).astype(jnp.bfloat16)
    for s in range(sources):
        wide_ref[s] = in_ref[s, 0:lines].astype(jnp.float32).reshape(rows, lanes)
    stats = jnp.concatenate([in_ref[s, lines] for s in range(sources)], 0)
    table_ref[...] = jnp.dot(stats, spread, preferred_element_type=jnp.float32)
    shared = None
    for start, size in blocks_of(lines):
        shape = (size, lanes)
        line = lax.broadcasted_iota(jnp.int32, shape, 0) + start
        fresh = shared is None or 8 % groups != 0 or shared[0].shape != shape
        zero = jnp.zeros(shape, jnp.float32)
        s_y, s_ty, s_zero, s_one, s_two = zero, zero, zero, zero, zero
        values = []
        for s in range(sources):
            for d in range(dates):

                def stat_at(b):
                    at = s * dates + d
                    row = table_ref[at : at + 1, b * lanes : (b + 1) * lanes]
                    return jnp.broadcast_to(row, shape)

                mean = stat_at(start // groups)
                for b in range(start // groups + 1, (start + size - 1) // groups + 1):
                    mean = jnp.where(line >= b * groups, stat_at(b), mean)
                value = wide_ref[s, pl.ds(start * dates + d, size, stride=dates), :]
                values.append(value)
                clear = value < limit
                year = stat_at(bands)
                part = jnp.where(clear, value - mean, 0.0)
                s_y = s_y + part
                s_ty = s_ty + year * part
                if fresh:
                    timed = jnp.where(clear, year, 0.0)
                    s_zero = s_zero + jnp.where(clear, 1.0, 0.0)
                    s_one = s_one + timed
                    s_two = s_two + timed * year
        median = middle_of(values, shape)
        if fresh:
            first = s_zero + ridge
            shared = (first, s_one, first * (s_two + ridge) - s_one * s_one)
        first, s_one, determinant = shared
        slope = (first * s_ty - s_one * s_y) / determinant
        for c in range(out_ref.shape[0]):
            out_ref[c, start : start + size, :] = median
            out_ref[c, lines + start : lines + start + size, :] = slope


def place_kernel(bands, groups, turns, pieces, in_ref, median_ref, slope_ref, held_ref, sems):
    lines = bands * groups
    source = {part: s for s, part in enumerate(turns)}
    share = len(turns) // pieces
    copies = []
    for piece in range(pieces):
        for n, to_ref in enumerate((median_ref, slope_ref)):
            for part in range(piece * share, (piece + 1) * share):
                for g in range(groups):
                    at = (part * groups + g) * lanes
                    line = in_ref[source[part], pl.ds(n * lines + g, bands, stride=groups), :]
                    held_ref[n, :, at : at + lanes] = line
            where = pl.ds(piece * share * groups * lanes, share * groups * lanes)
            copy = pltpu.make_async_copy(held_ref.at[n, :, where], to_ref.at[:, where], sems.at[n, piece])
            copy.start()
            copies.append(copy)
    for copy in copies:
        copy.wait()


def call(kernel, name, out_shape, in_specs, scratch=(), flops=0, aliases={}, space=pltpu.VMEM):
    many = isinstance(out_shape, tuple)
    spec = pl.BlockSpec(memory_space=space)
    cost = pl.CostEstimate(flops=flops, bytes_accessed=flops, transcendentals=0) if flops else None
    return pl.pallas_call(
        kernel,
        out_shape=out_shape,
        in_specs=[pl.BlockSpec(memory_space=space) for space in in_specs],
        out_specs=tuple([spec] * len(out_shape)) if many else spec,
        scratch_shapes=scratch,
        compiler_params=pltpu.CompilerParams(vmem_limit_bytes=8 * 1024 * 1024),
        cost_estimate=cost,
        input_output_aliases=aliases,
        name=name,
    )


def tuned(parts, tiles):
    return len(orders) == tiles and len(again) == parts


def exchange(x, turn, tiles):
    if not tuned(x.shape[0], tiles):
        return lax.all_to_all(x, "date", split_axis=0, concat_axis=0, tiled=True)
    groups = [[order[i] * tiles + tile for i in turn] for tile, order in enumerate(orders)]
    return lax.all_to_all(x, ("date", "pix"), split_axis=0, concat_axis=0, tiled=True, axis_index_groups=groups)


def local(parts, tiles, reflect, cloud_free, days):
    dates, bands, pixels = reflect.shape
    groups = pixels // parts // lanes
    lines = bands * groups
    rows = lines * dates
    inside, outside = pltpu.VMEM, pltpu.HBM
    array = jax.ShapeDtypeStruct
    values = jnp.transpose(reflect, (1, 0, 2))
    held, mask, own = call(
        functools.partial(load_kernel, bands),
        "load",
        (
            array(values.shape, values.dtype),
            array(cloud_free.shape, cloud_free.dtype),
            array((dates, lanes), jnp.float32),
        ),
        [outside if dates > 1 else pl.ANY, outside, outside],
        [pltpu.SMEM((dates,), jnp.int32), pltpu.SemaphoreType.DMA((3,))],
    )(*[pltpu.with_memory_space_constraint(x, outside) if x.size > 1 else x for x in (days, values, cloud_free)])
    if tiles == 2:
        other = lax.ppermute(own, "pix", [(0, 1), (1, 0)])
    else:
        ring = [(i, (i + 1) % tiles) for i in range(tiles)]
        passed, other = own, jnp.zeros(own.shape, own.dtype)
        for _ in range(tiles - 1):
            passed = lax.ppermute(passed, "pix", ring)
            other = other + passed
    packed = call(
        functools.partial(pack_kernel, bands, groups),
        "pack",
        array((parts, lines + 1, dates, lanes), jnp.bfloat16),
        [inside, inside],
        flops=16_000_000,
    )(held, mask)
    stamped = call(
        functools.partial(stamp_kernel, bands, lines),
        "stamp",
        array(packed.shape, packed.dtype),
        [inside] * 3,
        aliases={2: 0},
    )(own, other, pltpu.with_memory_space_constraint(packed, inside))
    turns = again if tuned(parts, tiles) else tuple(range(parts))
    moved = exchange(stamped, tuple(range(parts)), tiles)
    fitted = call(
        functools.partial(fit_kernel, bands, groups, dates),
        "fit",
        array((parts, 2 * lines, lanes), jnp.float32),
        [inside],
        [
            pltpu.VMEM((parts, rows, lanes), jnp.float32),
            pltpu.VMEM((parts * dates, (bands + 1) * lanes), jnp.float32),
        ],
    )(moved)
    spread = exchange(fitted, turns, tiles)
    shape = array((bands, pixels), jnp.float32)
    return call(
        functools.partial(place_kernel, bands, groups, turns, 2),
        "place",
        (shape, shape),
        [inside],
        [pltpu.VMEM((2, bands, pixels), jnp.float32), pltpu.SemaphoreType.DMA((2, 2))],
        space=outside,
    )(spread)


def solution(mesh):
    placed = (P("date", None, "pix"), P("date", "pix"), P("date"))
    return jax.shard_map(
        functools.partial(local, mesh.shape["date"], mesh.shape["pix"]),
        mesh=mesh,
        in_specs=placed,
        out_specs=(P(None, "pix"), P(None, "pix")),
        check_vma=False,
    )
```
